256 devices in a mesh: group: 32 (over z, y_hi, core), helper: 8 (over y_lo, x).
Axes of the slice: x: 4, y: 4 (y_hi: 2, y_lo: 2; y = y_hi * 2 + y_lo), z: 8, core: 2. Of those that a mesh axis runs over, the one named last changes fastest.
Arguments:
- candidates: bfloat16 [32, 2048, 1024], P('group', 'helper'), may hold values from -6 to 6
- prefix_cache: bfloat16 [32, 2, 3072, 1024], P('group', None, 'helper'), may hold values from -6 to 6
- w_uvqk: bfloat16 [1024, 4096], replicated, may hold values from -0.1875 to 0.1875
- w_output: bfloat16 [1024, 1024], replicated, may hold values from -0.1875 to 0.1875
- norm_gain: float32 [1024], replicated, may hold values from 0.1 to 1.9
- owner: int32 [32], replicated, may hold values from 0 to 31, as said below
- counts: int32 [32], replicated, may hold values from 1024 to 2048, as said below
- prefix_len: int32 [32], replicated, may hold values from 96 to 3072, as said below
Outputs:
- update: bfloat16 [32, 2048, 1024], P('group', 'helper')
The draws below stay inside these ranges and needn't reach their ends.
Inputs may be any that keep to these rules, and one draw needn't show every extreme that they name: owner[u] = (u + s) mod 32 for one shift s of the round. `counts`: multiples of 128; some user has exactly 2048. `prefix_len`: some user has exactly 3072.
All inputs are finite; a program needn't handle non-finite values.
Results may differ from the reference program's by a relative error of at most 0.012.
Values may be sent and summed in bfloat16 or wider, within the bound.
No kernel may reach another device: no remote copies, remote signals or barrier semaphores. Data moves between devices by JAX's collectives and lax.ppermute only.
A program may use at most 128 MiB of HBM per device.

```python
import jax
import jax.numpy as jnp
from jax import lax

D = 1024
HEADS = 8
PREFIX = 3072
CAND = 2048
GRAIN = 128
USERS = 32


def draw_owner(key, part):
    offset = jax.random.randint(key, (), 0, USERS)
    return ((jnp.arange(USERS, dtype=jnp.int32) + offset) % USERS).astype(jnp.int32)


def draw_counts(key, part):
    first, second = jax.random.split(jax.random.fold_in(key, 11))
    steps = jax.random.randint(first, (USERS,), CAND // (2 * GRAIN), CAND // GRAIN + 1)
    chosen = jax.random.randint(second, (), 0, USERS)
    values = jnp.where(jnp.arange(USERS) == chosen, CAND, steps * GRAIN)
    return values.astype(jnp.int32)


def draw_prefix_len(key, part):
    first, second = jax.random.split(jax.random.fold_in(key, 23))
    values = jax.random.randint(first, (USERS,), max(1, PREFIX // 32), PREFIX + 1)
    chosen = jax.random.randint(second, (), 0, USERS)
    values = jnp.where(jnp.arange(USERS) == chosen, PREFIX, values)
    return values.astype(jnp.int32)


def block_levels(own_key, dims, shards, smallest, high):
    def one(position, blocks):
        draws = jax.random.uniform(jax.random.fold_in(jax.random.fold_in(own_key, 6), position), (blocks,), jnp.float32, smallest / len(shards), high / len(shards))
        return jnp.repeat(jnp.exp(draws), dims[position] // blocks).reshape((-1,) + (1,) * (len(dims) - position - 1))

    factor_of = one(*shards[0])
    for cut in shards[1:]:
        factor_of = factor_of * one(*cut)
    return factor_of


def noise(stream_key, shape, scale, most, cuts=(), kind=jnp.bfloat16):
    level = block_levels(stream_key, shape, cuts, -0.22, 0.18) if cuts else 1.0
    values = jax.random.normal(stream_key, shape, jnp.float32) * scale * level
    return jnp.minimum(jnp.maximum(values, -most), most).astype(kind)


def setup_inputs(seed: int = 0) -> dict:
    seeds = jax.random.split(jax.random.key(seed), 9)
    candidates = noise(seeds[0], (USERS, CAND, D), 1.0, 6.0, ((0, 32), (1, 8)))
    prefix_cache = noise(seeds[1], (USERS, 2, PREFIX, D), 1.0, 6.0, ((0, 32), (2, 8)))
    w_uvqk = noise(seeds[2], (D, 4 * D), D ** -0.5, 0.1875)
    w_output = noise(seeds[3], (D, D), D ** -0.5, 0.1875)
    norm_gain = jnp.clip(1.0 + 0.18 * jax.random.normal(seeds[4], (D,), jnp.float32), 0.1, 1.9)
    owner = draw_owner(jax.random.fold_in(seeds[8], 71), 0)
    counts = draw_counts(jax.random.fold_in(seeds[8], 71), 0)
    prefix_len = draw_prefix_len(jax.random.fold_in(seeds[8], 71), 0)
    return dict(candidates=candidates, prefix_cache=prefix_cache, w_uvqk=w_uvqk, w_output=w_output, norm_gain=norm_gain, owner=owner, counts=counts, prefix_len=prefix_len)


def score_user(rows, keys, values, count, visible, w_uvqk, w_output, norm_gain):
    width = rows.shape[1]
    head = width // HEADS
    scale = head ** (-0.5)
    total = rows.shape[0]
    proj = jax.nn.silu(jnp.dot(rows, w_uvqk, preferred_element_type=jnp.float32))
    gate_u = proj[:, :width]
    own_v = proj[:, width:2 * width].astype(jnp.bfloat16).astype(jnp.float32).reshape(total, HEADS, head)
    query = proj[:, 2 * width:3 * width].astype(jnp.bfloat16).astype(jnp.float32).reshape(total, HEADS, head)
    own_k = proj[:, 3 * width:].astype(jnp.bfloat16).astype(jnp.float32).reshape(total, HEADS, head)
    length = keys.shape[0]
    keys4 = keys.astype(jnp.float32).reshape(length, HEADS, head)
    values4 = values.astype(jnp.float32).reshape(length, HEADS, head)
    scores = jnp.einsum('rhd,nhd->hrn', query, keys4) * scale
    allowed = jnp.arange(length, dtype=jnp.int32) < visible
    weights = jnp.where(allowed[None, None, :], jax.nn.silu(scores), 0.0).astype(jnp.bfloat16).astype(jnp.float32)
    mixed = jnp.einsum('hrn,nhd->rhd', weights, values4)
    selfw = jax.nn.silu(lax.optimization_barrier(jnp.sum(query * own_k, axis=-1)) * scale).astype(jnp.bfloat16).astype(jnp.float32)
    mixed = (mixed + selfw[:, :, None] * own_v).reshape(total, width)
    centre = mixed - lax.optimization_barrier(jnp.mean(mixed, axis=-1, keepdims=True))
    spread = lax.optimization_barrier(jnp.mean(centre * centre, axis=-1, keepdims=True))
    normed = (centre * lax.rsqrt(spread + 1e-05) * norm_gain * gate_u).astype(jnp.bfloat16)
    result = jnp.dot(normed, w_output, preferred_element_type=jnp.float32)
    live = jnp.arange(total, dtype=jnp.int32) < count
    return jnp.where(live[:, None], result, 0.0).astype(jnp.bfloat16)

def reference(candidates, prefix_cache, w_uvqk, w_output, norm_gain, owner, counts, prefix_len):
    shift = owner[0]

    def one_user(user):
        rows = lax.dynamic_index_in_dim(candidates, user, 0, keepdims=False)
        source = ((user + shift) % USERS).astype(jnp.int32)
        cache = lax.dynamic_index_in_dim(prefix_cache, source, 0, keepdims=False)
        count = lax.dynamic_index_in_dim(counts, user, 0, keepdims=False)
        visible = lax.dynamic_index_in_dim(prefix_len, user, 0, keepdims=False)
        return score_user(rows, cache[0], cache[1], count, visible, w_uvqk, w_output, norm_gain)
    result = lax.map(one_user, jnp.arange(USERS, dtype=jnp.int32))
    return jnp.roll(result, shift, axis=0)
```

```python
import functools

import jax
import jax.numpy as jnp
from jax import lax
from jax.experimental import pallas as pl
from jax.experimental.pallas import tpu as pltpu
from jax.sharding import PartitionSpec as P

HEADS = 8


def silu(value):
    half = 0.5 * value
    return half + half * jnp.tanh(half)


def exchange(value):
    return lax.all_to_all(value, "helper", 0, 0, tiled=True)


def shift_by(steps, count, head):
    pairs = [(source, (source + steps) % count) for source in range(count)]

    def move(tokens, cache):
        moved = lax.ppermute(tokens, "group", pairs) if steps else tokens
        return moved, exchange(split_heads(cache, head))

    return move


def limit(mebibytes):
    return pltpu.CompilerParams(vmem_limit_bytes=mebibytes << 20)


def split_heads_kernel(cache_ref, out_ref):
    out_ref[0] = cache_ref[...]


def split_heads(cache, head):
    two, length, width = cache.shape
    heads = width // head
    return pl.pallas_call(
        split_heads_kernel,
        grid=(heads,),
        in_specs=[pl.BlockSpec((two, length, head), lambda h: (0, 0, h))],
        out_specs=pl.BlockSpec((1, two, length, head), lambda h: (h, 0, 0, 0)),
        out_shape=jax.ShapeDtypeStruct((heads, two, length, head), cache.dtype),
        compiler_params=limit(4),
        name="split_heads",
    )(cache)


def query_kernel(tokens_ref, w_ref, out_ref):
    heads_here, _, head = out_ref.shape
    proj = jnp.dot(tokens_ref[...], w_ref[...], preferred_element_type=jnp.float32)
    proj = silu(proj).astype(jnp.bfloat16)
    for h in range(heads_here):
        out_ref[h] = proj[:, h * head : (h + 1) * head]


def project_query(tokens, w_uvqk, head):
    slots, width = tokens.shape
    heads = width // head
    cols = 4 * head
    per = cols // head
    steps = width // cols
    return pl.pallas_call(
        query_kernel,
        grid=(steps,),
        in_specs=[
            pl.BlockSpec((slots, width), lambda i: (0, 0)),
            pl.BlockSpec((width, cols), lambda i: (0, 2 * steps + i)),
        ],
        out_specs=pl.BlockSpec((per, slots, head), lambda i: (i, 0, 0)),
        out_shape=jax.ShapeDtypeStruct((heads, slots, head), jnp.bfloat16),
        cost_estimate=pl.CostEstimate(
            flops=2 * slots * width * width, bytes_accessed=2 * width * width, transcendentals=slots * width
        ),
        compiler_params=limit(8),
        name="project_query",
    )(tokens, w_uvqk)


def own_kernel(scale, tokens_ref, query_ref, wu_ref, wv_ref, wk_ref, gate_ref, own_ref):
    per, _, head = query_ref.shape
    tokens = tokens_ref[...]
    gate_ref[...] = silu(jnp.dot(tokens, wu_ref[...], preferred_element_type=jnp.float32))
    own_v = silu(jnp.dot(tokens, wv_ref[...], preferred_element_type=jnp.float32)).astype(jnp.bfloat16)
    own_k = silu(jnp.dot(tokens, wk_ref[...], preferred_element_type=jnp.float32)).astype(jnp.bfloat16)
    for h in range(per):
        cols = slice(h * head, (h + 1) * head)
        query = query_ref[h].astype(jnp.float32)
        score = jnp.sum(query * own_k[:, cols].astype(jnp.float32), axis=-1, keepdims=True) * scale
        weight = silu(score).astype(jnp.bfloat16).astype(jnp.float32)
        own_ref[h] = weight * own_v[:, cols].astype(jnp.float32)


def project_own(tokens, query, w_uvqk, head):
    slots, width = tokens.shape
    heads = width // head
    cols = 2 * head
    per = cols // head
    steps = width // cols
    return pl.pallas_call(
        functools.partial(own_kernel, head ** (-0.5)),
        grid=(steps,),
        in_specs=[
            pl.BlockSpec((slots, width), lambda i: (0, 0)),
            pl.BlockSpec((per, slots, head), lambda i: (i, 0, 0)),
            pl.BlockSpec((width, cols), lambda i: (0, i)),
            pl.BlockSpec((width, cols), lambda i: (0, steps + i)),
            pl.BlockSpec((width, cols), lambda i: (0, 3 * steps + i)),
        ],
        out_specs=[
            pl.BlockSpec((slots, cols), lambda i: (0, i)),
            pl.BlockSpec((per, slots, head), lambda i: (i, 0, 0)),
        ],
        out_shape=[
            jax.ShapeDtypeStruct((slots, width), jnp.float32),
            jax.ShapeDtypeStruct((heads, slots, head), jnp.float32),
        ],
        cost_estimate=pl.CostEstimate(
            flops=6 * slots * width * width, bytes_accessed=6 * width * width, transcendentals=3 * slots * width
        ),
        compiler_params=limit(16),
        name="project_own",
    )(tokens, query, w_uvqk, w_uvqk, w_uvqk)


def attend_kernel(scale, joined, meta_ref, query_ref, cache_ref, out_ref, keys_ref):
    blocks, slots, head = query_ref.shape
    shards, _, length, _ = cache_ref.shape
    span = joined * length
    count = meta_ref[0]
    visible = meta_ref[1]
    live_blocks = jnp.minimum((count + slots - 1) // slots, blocks)
    live_spans = jnp.minimum((visible + span - 1) // span, shards // joined)

    def clear_keys(shard, carry):
        place = shard * length + lax.broadcasted_iota(jnp.int32, (length, head), 0)
        keys = cache_ref[shard, 0].astype(jnp.float32)
        keys_ref[shard] = jnp.where(place < visible, keys, 0.0).astype(jnp.bfloat16)
        return carry

    lax.fori_loop(0, shards, clear_keys, 0)

    def row_block(number, carry):
        query = (query_ref[number].astype(jnp.float32) * (0.5 * scale)).astype(jnp.bfloat16)

        def span_block(part, acc):
            keys = keys_ref[pl.ds(part * joined, joined)].reshape(span, head)
            values = cache_ref[pl.ds(part * joined, joined), 1].reshape(span, head)
            half = lax.dot_general(
                query, keys, (((1,), (1,)), ((), ())), preferred_element_type=jnp.float32
            ).astype(jnp.bfloat16)
            weight = half + half * jnp.tanh(half)
            return acc + jnp.dot(weight, values, preferred_element_type=jnp.float32)

        acc = lax.fori_loop(0, live_spans, span_block, jnp.zeros((slots, head), jnp.float32))
        out_ref[number] = acc.astype(jnp.bfloat16)
        return carry

    lax.fori_loop(0, live_blocks, row_block, 0)

    def dead_block(number, carry):
        out_ref[number] = jnp.zeros((slots, head), jnp.bfloat16)
        return carry

    lax.fori_loop(live_blocks, blocks, dead_block, 0)


def attend(meta, query, cache):
    blocks, slots, head = query.shape
    shards, _, length, _ = cache.shape
    joined = 2 if shards % 2 == 0 else 1
    flops = 4 * blocks * slots * shards * length * head
    return pl.pallas_call(
        functools.partial(attend_kernel, head ** (-0.5), joined),
        grid_spec=pltpu.PrefetchScalarGridSpec(
            num_scalar_prefetch=1,
            grid=(1,),
            in_specs=[
                pl.BlockSpec(query.shape, lambda i, meta: (0, 0, 0)),
                pl.BlockSpec(cache.shape, lambda i, meta: (0, 0, 0, 0)),
            ],
            out_specs=pl.BlockSpec(query.shape, lambda i, meta: (0, 0, 0)),
            scratch_shapes=[pltpu.VMEM((shards, length, head), jnp.bfloat16)],
        ),
        out_shape=jax.ShapeDtypeStruct(query.shape, jnp.bfloat16),
        cost_estimate=pl.CostEstimate(
            flops=flops, bytes_accessed=cache.size * 2, transcendentals=blocks * slots * shards * length
        ),
        compiler_params=limit(16),
        name="attend",
    )(meta, query, cache)


def finish_kernel(meta_ref, mixed_ref, own_ref, gate_ref, gain_ref, w_ref, out_ref):
    heads, slots, head = mixed_ref.shape
    count = meta_ref[0]
    first = meta_ref[2] * slots
    width = heads * head
    mixed = jnp.concatenate(
        [mixed_ref[h].astype(jnp.float32) + own_ref[h] for h in range(heads)], axis=1
    )
    centre = mixed - jnp.sum(mixed, axis=-1, keepdims=True) * (1.0 / width)
    spread = jnp.sum(centre * centre, axis=-1, keepdims=True) * (1.0 / width)
    normed = (centre * lax.rsqrt(spread + 1e-05) * gain_ref[...] * gate_ref[...]).astype(jnp.bfloat16)
    result = jnp.dot(normed, w_ref[...], preferred_element_type=jnp.float32)
    place = first + lax.broadcasted_iota(jnp.int32, result.shape, 0)
    out_ref[...] = jnp.where(place < count, result, 0.0).astype(jnp.bfloat16)


def finish(meta, mixed, own, gate, gain, w_output):
    slots, width = gate.shape
    return pl.pallas_call(
        finish_kernel,
        grid_spec=pltpu.PrefetchScalarGridSpec(
            num_scalar_prefetch=1,
            grid=(1,),
            in_specs=[
                pl.BlockSpec(mixed.shape, lambda i, meta: (0, 0, 0)),
                pl.BlockSpec(own.shape, lambda i, meta: (0, 0, 0)),
                pl.BlockSpec(gate.shape, lambda i, meta: (0, 0)),
                pl.BlockSpec((1, width), lambda i, meta: (0, 0)),
                pl.BlockSpec(w_output.shape, lambda i, meta: (0, 0)),
            ],
            out_specs=pl.BlockSpec((slots, width), lambda i, meta: (0, 0)),
        ),
        out_shape=jax.ShapeDtypeStruct((slots, width), jnp.bfloat16),
        cost_estimate=pl.CostEstimate(
            flops=2 * slots * width * width, bytes_accessed=2 * width * width, transcendentals=slots
        ),
        compiler_params=limit(16),
        name="finish",
    )(meta, mixed, own, gate, gain.reshape(1, width), w_output)


def local(candidates, prefix_cache, w_uvqk, w_output, norm_gain, owner, counts, prefix_len):
    groups = lax.axis_size("group")
    group_here = lax.axis_index("group")
    helper_here = lax.axis_index("helper")
    offset = owner[0]
    width = candidates.shape[2]
    head = width // HEADS
    moves = [shift_by(steps, groups, head) for steps in range(groups)]
    tokens, cache = lax.switch(offset, moves, candidates[0], prefix_cache[0])
    user = (group_here - offset) % groups
    table = jnp.stack([counts, prefix_len, jnp.full_like(counts, helper_here)])
    places = lax.broadcasted_iota(jnp.int32, table.shape, 1)
    meta = jnp.sum(jnp.where(places == user, table, 0), axis=1)
    w_uvqk = pltpu.with_memory_space_constraint(w_uvqk, pltpu.HBM)
    query = project_query(tokens, w_uvqk, head)
    query_all = exchange(query)
    gate, own = project_own(tokens, query, w_uvqk, head)
    heads_out = attend(meta, query_all, cache)
    mixed = exchange(heads_out)
    return finish(meta, mixed, own, gate, norm_gain, w_output)[None]


def solution(mesh):
    in_specs = (
        P("group", "helper", None),
        P("group", None, "helper", None),
        P(),
        P(),
        P(),
        P(),
        P(),
        P(),
    )
    out_specs = P("group", "helper", None)
    return jax.shard_map(local, mesh=mesh, in_specs=in_specs, out_specs=out_specs, check_vma=False)
```

```python
import functools

import jax
import jax.numpy as jnp
from jax import lax
from jax.experimental import pallas as pl
from jax.experimental.pallas import tpu as pltpu
from jax.sharding import PartitionSpec as P


HEADS = 8


def silu(value):
    half = 0.5 * value
    return half + half * jnp.tanh(half)


def exchange(value):
    return lax.all_to_all(value, "helper", 0, 0, tiled=True)


def fetch_kernel(w_uvqk_ref, query_ref, sem):
    width = query_ref.shape[1]
    copy = pltpu.make_async_copy(w_uvqk_ref.at[:, 2 * width : 3 * width], query_ref, sem)
    copy.start()
    copy.wait()


def fetch(w_uvqk):
    width = w_uvqk.shape[0]
    return pl.pallas_call(
        fetch_kernel,
        in_specs=[pl.BlockSpec(memory_space=pl.ANY)],
        out_specs=pl.BlockSpec(memory_space=pltpu.VMEM),
        out_shape=pltpu.VMEM((width, width), w_uvqk.dtype),
        scratch_shapes=[pltpu.SemaphoreType.DMA],
        compiler_params=limit(1),
        name="fetch",
    )(w_uvqk)


def shift_by(steps, count, head):
    pairs = [(source, (source + steps) % count) for source in range(count)]

    def move(tokens, cache, w_uvqk):
        moved = lax.ppermute(tokens, "group", pairs) if steps else tokens
        split = split_heads(cache, head)
        cache = exchange(split)
        w_query = fetch(w_uvqk)
        return moved, cache, w_query

    return move


def limit(mebibytes):
    return pltpu.CompilerParams(vmem_limit_bytes=mebibytes << 20)


def split_heads_kernel(cache_ref, out_ref):
    out_ref[0] = cache_ref[...]


def split_heads(cache, head):
    two, length, width = cache.shape
    heads = width // head
    return pl.pallas_call(
        split_heads_kernel,
        grid=(heads,),
        in_specs=[pl.BlockSpec((two, length, head), lambda h: (0, 0, h))],
        out_specs=pl.BlockSpec((1, two, length, head), lambda h: (h, 0, 0, 0)),
        out_shape=jax.ShapeDtypeStruct((heads, two, length, head), cache.dtype),
        compiler_params=limit(4),
        name="split_heads",
    )(cache)


def query_kernel(tokens_ref, w_ref, out_ref):
    heads, _, head = out_ref.shape
    tokens = tokens_ref[...]
    for h in range(0, heads, 2):
        cols = slice(h * head, (h + 2) * head)
        proj = jnp.dot(tokens, w_ref[:, cols], preferred_element_type=jnp.float32)
        proj = silu(proj).astype(jnp.bfloat16)
        out_ref[h] = proj[:, :head]
        out_ref[h + 1] = proj[:, head:]


def project_query(tokens, w_query, head):
    slots, width = tokens.shape
    heads = width // head
    return pl.pallas_call(
        query_kernel,
        out_shape=jax.ShapeDtypeStruct((heads, slots, head), jnp.bfloat16),
        cost_estimate=pl.CostEstimate(
            flops=2 * slots * width * width, bytes_accessed=2 * width * width, transcendentals=slots * width
        ),
        compiler_params=limit(8),
        name="project_query",
    )(tokens, w_query)


def own_kernel(scale, tokens_ref, query_ref, wu_ref, wv_ref, wk_ref, gate_ref, own_ref):
    per, _, head = query_ref.shape
    tokens = tokens_ref[...]
    gate_ref[...] = silu(jnp.dot(tokens, wu_ref[...], preferred_element_type=jnp.float32))
    own_v = silu(jnp.dot(tokens, wv_ref[...], preferred_element_type=jnp.float32)).astype(jnp.bfloat16)
    own_k = silu(jnp.dot(tokens, wk_ref[...], preferred_element_type=jnp.float32)).astype(jnp.bfloat16)
    for h in range(per):
        cols = slice(h * head, (h + 1) * head)
        query = query_ref[h].astype(jnp.float32)
        score = jnp.sum(query * own_k[:, cols].astype(jnp.float32), axis=-1, keepdims=True) * scale
        weight = silu(score).astype(jnp.bfloat16).astype(jnp.float32)
        own_ref[h] = weight * own_v[:, cols].astype(jnp.float32)


def project_own(tokens, query, w_uvqk, head):
    slots, width = tokens.shape
    heads = width // head
    cols = 2 * head
    per = cols // head
    steps = width // cols
    return pl.pallas_call(
        functools.partial(own_kernel, head ** (-0.5)),
        grid=(steps,),
        in_specs=[
            pl.BlockSpec((slots, width), lambda i: (0, 0)),
            pl.BlockSpec((per, slots, head), lambda i: (i, 0, 0)),
            pl.BlockSpec((width, cols), lambda i: (0, i)),
            pl.BlockSpec((width, cols), lambda i: (0, steps + i)),
            pl.BlockSpec((width, cols), lambda i: (0, 3 * steps + i)),
        ],
        out_specs=[
            pl.BlockSpec((slots, cols), lambda i: (0, i)),
            pl.BlockSpec((per, slots, head), lambda i: (i, 0, 0)),
        ],
        out_shape=[
            jax.ShapeDtypeStruct((slots, width), jnp.float32),
            jax.ShapeDtypeStruct((heads, slots, head), jnp.float32),
        ],
        cost_estimate=pl.CostEstimate(
            flops=6 * slots * width * width, bytes_accessed=6 * width * width, transcendentals=3 * slots * width
        ),
        compiler_params=limit(16),
        name="project_own",
    )(tokens, query, w_uvqk, w_uvqk, w_uvqk)


def attend_kernel(scale, rows, chunk, groups, meta_ref, query_ref, cache_ref, out_ref, keys_ref):
    blocks, slots, head = query_ref.shape
    shards, _, length, _ = cache_ref.shape
    per = rows // slots
    count = meta_ref[0]
    visible = meta_ref[1]
    live_blocks = jnp.minimum((count + rows - 1) // rows, blocks // per)

    def clear_keys(shard, carry):
        place = shard * length + lax.broadcasted_iota(jnp.int32, (length, head), 0)
        keys = cache_ref[shard, 0].astype(jnp.float32)
        keys_ref[shard] = jnp.where(place < visible, keys, 0.0).astype(jnp.bfloat16)
        return carry

    lax.fori_loop(0, shards, clear_keys, 0)

    def attend_to(used):
        span = used * length
        pieces = span // chunk

        def row_block(number, carry):
            first = number * per
            query = query_ref[pl.ds(first, per)].reshape(rows, head)
            query = (query.astype(jnp.float32) * (0.5 * scale)).astype(jnp.bfloat16)
            keys = keys_ref[:used].reshape(span, head)
            values = cache_ref[:used, 1].reshape(span, head)

            def scores(piece):
                part = keys[piece * chunk : (piece + 1) * chunk]
                return lax.dot_general(
                    query, part, (((1,), (1,)), ((), ())), preferred_element_type=jnp.float32
                )

            acc = jnp.zeros((rows, head), jnp.float32)
            ahead = scores(0)
            for piece in range(pieces):
                half = ahead.astype(jnp.bfloat16)
                if piece + 1 < pieces:
                    ahead = scores(piece + 1)
                weight = half + half * jnp.tanh(half)
                part = values[piece * chunk : (piece + 1) * chunk]
                acc = acc + jnp.dot(weight, part, preferred_element_type=jnp.float32)
            out_ref[pl.ds(first, per)] = acc.astype(jnp.bfloat16).reshape(per, slots, head)
            return carry

        lax.fori_loop(0, live_blocks, row_block, 0)

    below = 0
    for used in groups:
        within = visible > below * length
        if used < shards:
            within = jnp.logical_and(within, visible <= used * length)
        pl.when(within)(functools.partial(attend_to, used))
        below = used

    def dead_block(number, carry):
        out_ref[pl.ds(number * per, per)] = jnp.zeros((per, slots, head), jnp.bfloat16)
        return carry

    lax.fori_loop(live_blocks, blocks // per, dead_block, 0)


def attend(meta, query, cache):
    blocks, slots, head = query.shape
    shards, _, length, _ = cache.shape
    rows = 2 * slots
    chunk = length
    groups = (shards // 2, shards)
    flops = 4 * blocks * slots * shards * length * head
    return pl.pallas_call(
        functools.partial(attend_kernel, head ** (-0.5), rows, chunk, groups),
        grid_spec=pltpu.PrefetchScalarGridSpec(
            num_scalar_prefetch=1,
            grid=(1,),
            in_specs=[
                pl.BlockSpec(query.shape, lambda i, meta: (0, 0, 0)),
                pl.BlockSpec(cache.shape, lambda i, meta: (0, 0, 0, 0)),
            ],
            out_specs=pl.BlockSpec(query.shape, lambda i, meta: (0, 0, 0)),
            scratch_shapes=[pltpu.VMEM((shards, length, head), jnp.bfloat16)],
        ),
        out_shape=jax.ShapeDtypeStruct(query.shape, jnp.bfloat16),
        cost_estimate=pl.CostEstimate(
            flops=flops, bytes_accessed=cache.size * 2, transcendentals=blocks * slots * shards * length
        ),
        compiler_params=limit(24),
        name="attend",
    )(meta, query, cache)


def finish_kernel(meta_ref, mixed_ref, own_ref, gate_ref, gain_ref, w_ref, out_ref):
    heads, slots, head = mixed_ref.shape
    count = meta_ref[0]
    first = meta_ref[2] * slots
    width = heads * head
    mixed = jnp.concatenate(
        [mixed_ref[h].astype(jnp.float32) + own_ref[h] for h in range(heads)], axis=1
    )
    centre = mixed - jnp.sum(mixed, axis=-1, keepdims=True) * (1.0 / width)
    spread = jnp.sum(centre * centre, axis=-1, keepdims=True) * (1.0 / width)
    normed = (centre * lax.rsqrt(spread + 1e-05) * gain_ref[...] * gate_ref[...]).astype(jnp.bfloat16)
    result = jnp.dot(normed, w_ref[...], preferred_element_type=jnp.float32)
    place = first + lax.broadcasted_iota(jnp.int32, result.shape, 0)
    out_ref[...] = jnp.where(place < count, result, 0.0).astype(jnp.bfloat16)


def finish(meta, mixed, own, gate, gain, w_output):
    slots, width = gate.shape
    return pl.pallas_call(
        finish_kernel,
        grid_spec=pltpu.PrefetchScalarGridSpec(
            num_scalar_prefetch=1,
            grid=(1,),
            in_specs=[
                pl.BlockSpec(mixed.shape, lambda i, meta: (0, 0, 0)),
                pl.BlockSpec(own.shape, lambda i, meta: (0, 0, 0)),
                pl.BlockSpec(gate.shape, lambda i, meta: (0, 0)),
                pl.BlockSpec((1, width), lambda i, meta: (0, 0)),
                pl.BlockSpec(w_output.shape, lambda i, meta: (0, 0)),
            ],
            out_specs=pl.BlockSpec((slots, width), lambda i, meta: (0, 0)),
        ),
        out_shape=jax.ShapeDtypeStruct((slots, width), jnp.bfloat16),
        cost_estimate=pl.CostEstimate(
            flops=2 * slots * width * width, bytes_accessed=2 * width * width, transcendentals=slots
        ),
        compiler_params=limit(16),
        name="finish",
    )(meta, mixed, own, gate, gain.reshape(1, width), w_output)


def local(candidates, prefix_cache, w_uvqk, w_output, norm_gain, owner, counts, prefix_len):
    groups = lax.axis_size("group")
    group_here = lax.axis_index("group")
    helper_here = lax.axis_index("helper")
    offset = owner[0]
    width = candidates.shape[2]
    head = width // HEADS
    moves = [shift_by(steps, groups, head) for steps in range(groups)]
    user = (group_here - offset) % groups
    table = jnp.stack([counts, prefix_len, jnp.full_like(counts, helper_here)])
    places = lax.broadcasted_iota(jnp.int32, table.shape, 1)
    meta = jnp.sum(jnp.where(places == user, table, 0), axis=1)
    w_uvqk = pltpu.with_memory_space_constraint(w_uvqk, pltpu.HBM)
    tokens, cache, w_query = lax.switch(
        offset, moves, candidates[0], prefix_cache[0], w_uvqk
    )
    query = project_query(tokens, w_query, head)
    query_all = exchange(query)
    gate, own = project_own(tokens, query, w_uvqk, head)
    heads_out = attend(meta, query_all, cache)
    mixed = exchange(heads_out)
    return finish(meta, mixed, own, gate, norm_gain, w_output)[None]


def solution(mesh):
    in_specs = (
        P("group", "helper", None),
        P("group", None, "helper", None),
        P(),
        P(),
        P(),
        P(),
        P(),
        P(),
    )
    out_specs = P("group", "helper", None)
    return jax.shard_map(local, mesh=mesh, in_specs=in_specs, out_specs=out_specs, check_vma=False)
```

```python
import functools

import jax
import jax.numpy as jnp
from jax import lax
from jax.experimental import pallas as pl
from jax.experimental.pallas import tpu as pltpu
from jax.sharding import PartitionSpec as P


HEADS = 8
FAR = 4


def silu(value):
    half = 0.5 * value
    return half + half * jnp.tanh(half)


def exchange(value):
    return lax.all_to_all(value, "helper", 0, 0, tiled=True)


def rotate(value, steps, count):
    if steps % count == 0:
        return value
    pairs = [(source, (source + steps) % count) for source in range(count)]
    return lax.ppermute(value, "group", pairs)


def near_move(steps, count, head):
    def move(tokens, cache, w_uvqk):
        moved = rotate(tokens, steps, count)
        split, w_query = prepare(cache, w_uvqk, head)
        return moved, split, w_query

    return move


def far_move(steps, count):
    def move(tokens, split):
        moved = rotate(tokens, steps, count)
        cache = exchange(split)
        return moved, cache

    return move


def route(offset, groups):
    signed = jnp.where(offset > groups // 2, offset - groups, offset)
    size = jnp.abs(signed)
    sign = jnp.where(signed < 0, -1, 1)
    most = groups // 2
    over = size > most - FAR
    near = jnp.where(over, size - most, size % FAR)
    far = jnp.where(over, most // FAR, size // FAR)
    return sign * near, sign * far


def limit(mebibytes):
    return pltpu.CompilerParams(vmem_limit_bytes=mebibytes << 20)


def prepare_kernel(cache_ref, w_uvqk_ref, split_ref, query_ref, sems):
    heads, _, _, head = split_ref.shape
    width = query_ref.shape[1]
    copies = [
        pltpu.make_async_copy(cache_ref.at[:, :, h * head : (h + 1) * head], split_ref.at[h], sems.at[h])
        for h in range(heads)
    ]
    copies.append(
        pltpu.make_async_copy(w_uvqk_ref.at[:, 2 * width : 3 * width], query_ref, sems.at[heads])
    )
    for copy in copies:
        copy.start()
    for copy in copies:
        copy.wait()


def prepare(cache, w_uvqk, head):
    two, length, width = cache.shape
    heads = width // head
    return pl.pallas_call(
        prepare_kernel,
        in_specs=[pl.BlockSpec(memory_space=pltpu.HBM), pl.BlockSpec(memory_space=pltpu.HBM)],
        out_specs=[pl.BlockSpec(memory_space=pltpu.VMEM), pl.BlockSpec(memory_space=pltpu.VMEM)],
        out_shape=[
            pltpu.VMEM((heads, two, length, head), cache.dtype),
            pltpu.VMEM((width, width), w_uvqk.dtype),
        ],
        scratch_shapes=[pltpu.SemaphoreType.DMA((heads + 1,))],
        compiler_params=limit(4),
        name="prepare",
    )(cache, w_uvqk)


def query_kernel(tokens_ref, w_ref, out_ref):
    heads, _, head = out_ref.shape
    tokens = tokens_ref[...]
    for h in range(0, heads, 2):
        cols = slice(h * head, (h + 2) * head)
        proj = jnp.dot(tokens, w_ref[:, cols], preferred_element_type=jnp.float32)
        proj = silu(proj).astype(jnp.bfloat16)
        out_ref[h] = proj[:, :head]
        out_ref[h + 1] = proj[:, head:]


def project_query(tokens, w_query, head):
    slots, width = tokens.shape
    heads = width // head
    return pl.pallas_call(
        query_kernel,
        out_shape=jax.ShapeDtypeStruct((heads, slots, head), jnp.bfloat16),
        cost_estimate=pl.CostEstimate(
            flops=2 * slots * width * width, bytes_accessed=2 * width * width, transcendentals=slots * width
        ),
        compiler_params=limit(8),
        name="project_query",
    )(tokens, w_query)


def own_kernel(scale, tokens_ref, query_ref, wu_ref, wv_ref, wk_ref, gate_ref, own_ref):
    per, _, head = query_ref.shape
    tokens = tokens_ref[...]
    gate_ref[...] = silu(jnp.dot(tokens, wu_ref[...], preferred_element_type=jnp.float32))
    own_v = silu(jnp.dot(tokens, wv_ref[...], preferred_element_type=jnp.float32)).astype(jnp.bfloat16)
    own_k = silu(jnp.dot(tokens, wk_ref[...], preferred_element_type=jnp.float32)).astype(jnp.bfloat16)
    for h in range(per):
        cols = slice(h * head, (h + 1) * head)
        query = query_ref[h].astype(jnp.float32)
        score = jnp.sum(query * own_k[:, cols].astype(jnp.float32), axis=-1, keepdims=True) * scale
        weight = silu(score).astype(jnp.bfloat16).astype(jnp.float32)
        own_ref[h] = weight * own_v[:, cols].astype(jnp.float32)


def project_own(tokens, query, w_uvqk, head):
    slots, width = tokens.shape
    heads = width // head
    cols = 2 * head
    per = cols // head
    steps = width // cols
    return pl.pallas_call(
        functools.partial(own_kernel, head ** (-0.5)),
        grid=(steps,),
        in_specs=[
            pl.BlockSpec((slots, width), lambda i: (0, 0)),
            pl.BlockSpec((per, slots, head), lambda i: (i, 0, 0)),
            pl.BlockSpec((width, cols), lambda i: (0, i)),
            pl.BlockSpec((width, cols), lambda i: (0, steps + i)),
            pl.BlockSpec((width, cols), lambda i: (0, 3 * steps + i)),
        ],
        out_specs=[
            pl.BlockSpec((slots, cols), lambda i: (0, i)),
            pl.BlockSpec((per, slots, head), lambda i: (i, 0, 0)),
        ],
        out_shape=[
            jax.ShapeDtypeStruct((slots, width), jnp.float32),
            jax.ShapeDtypeStruct((heads, slots, head), jnp.float32),
        ],
        cost_estimate=pl.CostEstimate(
            flops=6 * slots * width * width, bytes_accessed=6 * width * width, transcendentals=3 * slots * width
        ),
        compiler_params=limit(16),
        name="project_own",
    )(tokens, query, w_uvqk, w_uvqk, w_uvqk)


def attend_kernel(scale, rows, chunk, groups, meta_ref, query_ref, cache_ref, out_ref, keys_ref):
    blocks, slots, head = query_ref.shape
    shards, _, length, _ = cache_ref.shape
    per = rows // slots
    count = meta_ref[0]
    visible = meta_ref[1]
    live_blocks = jnp.minimum((count + rows - 1) // rows, blocks // per)

    def clear_keys(shard, carry):
        place = shard * length + lax.broadcasted_iota(jnp.int32, (length, head), 0)
        keys = cache_ref[shard, 0].astype(jnp.float32)
        keys_ref[shard] = jnp.where(place < visible, keys, 0.0).astype(jnp.bfloat16)
        return carry

    lax.fori_loop(0, shards, clear_keys, 0)

    def attend_to(used):
        span = used * length
        pieces = span // chunk

        def row_block(number, carry):
            first = number * per
            query = query_ref[pl.ds(first, per)].reshape(rows, head)
            query = (query.astype(jnp.float32) * (0.5 * scale)).astype(jnp.bfloat16)
            keys = keys_ref[:used].reshape(span, head)
            values = cache_ref[:used, 1].reshape(span, head)

            def scores(piece):
                part = keys[piece * chunk : (piece + 1) * chunk]
                return lax.dot_general(
                    query, part, (((1,), (1,)), ((), ())), preferred_element_type=jnp.float32
                )

            acc = jnp.zeros((rows, head), jnp.float32)
            ahead = scores(0)
            for piece in range(pieces):
                half = ahead.astype(jnp.bfloat16)
                if piece + 1 < pieces:
                    ahead = scores(piece + 1)
                weight = half + half * jnp.tanh(half)
                part = values[piece * chunk : (piece + 1) * chunk]
                acc = acc + jnp.dot(weight, part, preferred_element_type=jnp.float32)
            out_ref[pl.ds(first, per)] = acc.astype(jnp.bfloat16).reshape(per, slots, head)
            return carry

        lax.fori_loop(0, live_blocks, row_block, 0)

    below = 0
    for used in groups:
        within = visible > below * length
        if used < shards:
            within = jnp.logical_and(within, visible <= used * length)
        pl.when(within)(functools.partial(attend_to, used))
        below = used

    def dead_block(number, carry):
        out_ref[pl.ds(number * per, per)] = jnp.zeros((per, slots, head), jnp.bfloat16)
        return carry

    lax.fori_loop(live_blocks, blocks // per, dead_block, 0)


def attend(meta, query, cache):
    blocks, slots, head = query.shape
    shards, _, length, _ = cache.shape
    rows = 2 * slots
    chunk = length
    groups = (shards // 2, shards)
    flops = 4 * blocks * slots * shards * length * head
    return pl.pallas_call(
        functools.partial(attend_kernel, head ** (-0.5), rows, chunk, groups),
        grid_spec=pltpu.PrefetchScalarGridSpec(
            num_scalar_prefetch=1,
            grid=(1,),
            in_specs=[
                pl.BlockSpec(query.shape, lambda i, meta: (0, 0, 0)),
                pl.BlockSpec(cache.shape, lambda i, meta: (0, 0, 0, 0)),
            ],
            out_specs=pl.BlockSpec(query.shape, lambda i, meta: (0, 0, 0)),
            scratch_shapes=[pltpu.VMEM((shards, length, head), jnp.bfloat16)],
        ),
        out_shape=jax.ShapeDtypeStruct(query.shape, jnp.bfloat16),
        cost_estimate=pl.CostEstimate(
            flops=flops, bytes_accessed=cache.size * 2, transcendentals=blocks * slots * shards * length
        ),
        compiler_params=limit(24),
        name="attend",
    )(meta, query, cache)


def finish_kernel(pieces, meta_ref, mixed_ref, own_ref, gate_ref, gain_ref, w_ref, out_ref):
    heads, slots, head = mixed_ref.shape
    count = meta_ref[0]
    first = meta_ref[2] * slots
    width = heads * head
    rows = slots // pieces
    for piece in range(pieces):
        here = slice(piece * rows, (piece + 1) * rows)
        mixed = jnp.concatenate(
            [mixed_ref[h, here].astype(jnp.float32) + own_ref[h, here] for h in range(heads)], axis=1
        )
        centre = mixed - jnp.sum(mixed, axis=-1, keepdims=True) * (1.0 / width)
        spread = jnp.sum(centre * centre, axis=-1, keepdims=True) * (1.0 / width)
        normed = centre * lax.rsqrt(spread + 1e-05) * gain_ref[...] * gate_ref[here]
        result = jnp.dot(normed.astype(jnp.bfloat16), w_ref[...], preferred_element_type=jnp.float32)
        place = first + piece * rows + lax.broadcasted_iota(jnp.int32, result.shape, 0)
        out_ref[here] = jnp.where(place < count, result, 0.0).astype(jnp.bfloat16)


def finish(meta, mixed, own, gate, gain, w_output):
    slots, width = gate.shape
    return pl.pallas_call(
        functools.partial(finish_kernel, 2),
        grid_spec=pltpu.PrefetchScalarGridSpec(
            num_scalar_prefetch=1,
            grid=(1,),
            in_specs=[
                pl.BlockSpec(mixed.shape, lambda i, meta: (0, 0, 0)),
                pl.BlockSpec(own.shape, lambda i, meta: (0, 0, 0)),
                pl.BlockSpec(gate.shape, lambda i, meta: (0, 0)),
                pl.BlockSpec((1, width), lambda i, meta: (0, 0)),
                pl.BlockSpec(w_output.shape, lambda i, meta: (0, 0)),
            ],
            out_specs=pl.BlockSpec((slots, width), lambda i, meta: (0, 0)),
        ),
        out_shape=jax.ShapeDtypeStruct((slots, width), jnp.bfloat16),
        cost_estimate=pl.CostEstimate(
            flops=2 * slots * width * width, bytes_accessed=2 * width * width, transcendentals=slots
        ),
        compiler_params=limit(16),
        name="finish",
    )(meta, mixed, own, gate, gain.reshape(1, width), w_output)


def local(candidates, prefix_cache, w_uvqk, w_output, norm_gain, owner, counts, prefix_len):
    groups = lax.axis_size("group")
    group_here = lax.axis_index("group")
    helper_here = lax.axis_index("helper")
    offset = owner[0]
    width = candidates.shape[2]
    head = width // HEADS
    near, far = route(offset, groups)
    reach = groups // 2 // FAR
    nears = range(1 - FAR, FAR)
    fars = range(-reach, reach + 1)
    near_moves = [near_move(steps, groups, head) for steps in nears]
    far_moves = [far_move(FAR * steps, groups) for steps in fars]
    w_uvqk = pltpu.with_memory_space_constraint(w_uvqk, pltpu.HBM)
    prefix = pltpu.with_memory_space_constraint(prefix_cache[0], pltpu.HBM)
    tokens, split, w_query = lax.switch(near + FAR - 1, near_moves, candidates[0], prefix, w_uvqk)
    tokens, cache = lax.switch(far + reach, far_moves, tokens, split)
    user = (group_here - offset) % groups
    table = jnp.stack([counts, prefix_len, jnp.full_like(counts, helper_here)])
    places = lax.broadcasted_iota(jnp.int32, table.shape, 1)
    meta = jnp.sum(jnp.where(places == user, table, 0), axis=1)
    query = project_query(tokens, w_query, head)
    query_all = exchange(query)
    gate, own = project_own(tokens, query, w_uvqk, head)
    heads_out = attend(meta, query_all, cache)
    mixed = exchange(heads_out)
    return finish(meta, mixed, own, gate, norm_gain, w_output)[None]


def solution(mesh):
    in_specs = (
        P("group", "helper", None),
        P("group", None, "helper", None),
        P(),
        P(),
        P(),
        P(),
        P(),
        P(),
    )
    out_specs = P("group", "helper", None)
    return jax.shard_map(local, mesh=mesh, in_specs=in_specs, out_specs=out_specs, check_vma=False)
```

```python
import functools

import jax
import jax.numpy as jnp
from jax import lax
from jax.experimental import pallas as pl
from jax.experimental.pallas import tpu as pltpu
from jax.sharding import PartitionSpec as P


HEADS = 8
FAR = 4


def silu(value):
    half = 0.5 * value
    return half + half * jnp.tanh(half)


def exchange(value):
    return lax.all_to_all(value, "helper", 0, 0, tiled=True)


def rotate(value, steps, count):
    if steps % count == 0:
        return value
    pairs = [(source, (source + steps) % count) for source in range(count)]
    return lax.ppermute(value, "group", pairs)


def near_move(steps, count, head):
    def move(tokens, cache, w_uvqk):
        moved = rotate(tokens, steps, count)
        split, w_query = prepare(cache, w_uvqk, head)
        return moved, split, w_query

    return move


def far_move(steps, count, head):
    def move(tokens, split, w_query):
        moved = rotate(tokens, steps, count)
        cache = exchange(split)
        kept, query = project_query(moved, w_query, head)
        return kept, cache, query

    return move


def route(offset, groups):
    half = groups // 2
    bits = FAR.bit_length() - 1
    far = jnp.where(
        offset <= half - FAR,
        offset >> bits,
        jnp.where(offset < half + FAR, half // FAR, (offset + FAR - 1) >> bits),
    )
    return offset - FAR * far, far


def limit(mebibytes):
    return pltpu.CompilerParams(vmem_limit_bytes=mebibytes << 20)


def prepare_kernel(cache_ref, w_uvqk_ref, split_ref, query_ref, buf, reads, writes, sem):
    heads, _, _, head = split_ref.shape
    width = query_ref.shape[1]

    def pull(h):
        cols = pl.ds(pl.multiple_of(h * head, head), head)
        return pltpu.make_async_copy(cache_ref.at[:, :, cols], buf.at[h], reads.at[h])

    def push(h):
        return pltpu.make_async_copy(buf.at[h], split_ref.at[h], writes.at[h])

    def each(step):
        def body(h, carry):
            step(h)
            return carry

        lax.fori_loop(0, heads, body, 0)

    def pass_on(h):
        pull(h).wait()
        push(h).start()

    weights = pltpu.make_async_copy(w_uvqk_ref.at[:, 2 * width : 3 * width], query_ref, sem)
    each(lambda h: pull(h).start())
    weights.start()
    each(pass_on)
    each(lambda h: push(h).wait())
    weights.wait()


def prepare(cache, w_uvqk, head):
    two, length, width = cache.shape
    heads = width // head
    shape = (heads, two, length, head)
    return pl.pallas_call(
        prepare_kernel,
        in_specs=[pl.BlockSpec(memory_space=pltpu.HBM), pl.BlockSpec(memory_space=pltpu.HBM)],
        out_specs=[pl.BlockSpec(memory_space=pltpu.HBM), pl.BlockSpec(memory_space=pltpu.VMEM)],
        out_shape=[
            jax.ShapeDtypeStruct(shape, cache.dtype),
            pltpu.VMEM((width, width), w_uvqk.dtype),
        ],
        scratch_shapes=[
            pltpu.VMEM(shape, cache.dtype),
            pltpu.SemaphoreType.DMA((heads,)),
            pltpu.SemaphoreType.DMA((heads,)),
            pltpu.SemaphoreType.DMA,
        ],
        compiler_params=limit(3),
        name="prepare",
    )(cache, w_uvqk)


def query_kernel(tokens_ref, w_ref, kept_ref, out_ref, sem):
    heads, _, head = out_ref.shape
    keep = pltpu.make_async_copy(tokens_ref, kept_ref, sem)
    keep.start()
    tokens = tokens_ref[...]
    for h in range(0, heads, 2):
        cols = slice(h * head, (h + 2) * head)
        proj = jnp.dot(tokens, w_ref[:, cols], preferred_element_type=jnp.float32)
        proj = silu(proj).astype(jnp.bfloat16)
        out_ref[h] = proj[:, :head]
        out_ref[h + 1] = proj[:, head:]
    keep.wait()


def project_query(tokens, w_query, head):
    slots, width = tokens.shape
    heads = width // head
    whole = pl.BlockSpec(memory_space=pltpu.VMEM)
    return pl.pallas_call(
        query_kernel,
        in_specs=[whole, whole],
        out_specs=[pl.BlockSpec(memory_space=pltpu.HBM), whole],
        out_shape=[
            jax.ShapeDtypeStruct(tokens.shape, tokens.dtype),
            jax.ShapeDtypeStruct((heads, slots, head), jnp.bfloat16),
        ],
        scratch_shapes=[pltpu.SemaphoreType.DMA],
        cost_estimate=pl.CostEstimate(
            flops=2 * slots * width * width, bytes_accessed=2 * width * width, transcendentals=slots * width
        ),
        compiler_params=limit(8),
        name="project_query",
    )(tokens, w_query)


def own_kernel(scale, pieces, tokens_ref, query_ref, gain_ref, w_ref, gate_ref, own_ref, weights, sems):
    heads, _, head = query_ref.shape
    width = heads * head
    cols = width // pieces
    per = cols // head
    places = (0, 1, 3)

    def pull(piece, part):
        first = places[part] * width + piece * cols
        return pltpu.make_async_copy(
            w_ref.at[:, first : first + cols],
            weights.at[part, :, piece * cols : (piece + 1) * cols],
            sems.at[piece, part],
        )

    for piece in range(pieces):
        for part in (1, 2, 0):
            pull(piece, part).start()
    tokens = tokens_ref[...]

    def project(piece, part):
        pull(piece, part).wait()
        here = weights[part, :, piece * cols : (piece + 1) * cols]
        return silu(jnp.dot(tokens, here, preferred_element_type=jnp.float32))

    for piece in range(pieces):
        here = slice(piece * cols, (piece + 1) * cols)
        own_v = project(piece, 1).astype(jnp.bfloat16)
        own_k = project(piece, 2).astype(jnp.bfloat16)
        gate_ref[:, here] = (project(piece, 0) * gain_ref[:, here]).astype(gate_ref.dtype)
        for h in range(per):
            part = slice(h * head, (h + 1) * head)
            query = query_ref[piece * per + h].astype(jnp.float32)
            score = jnp.sum(query * own_k[:, part].astype(jnp.float32), axis=-1, keepdims=True) * scale
            weight = silu(score).astype(jnp.bfloat16).astype(jnp.float32)
            term = weight * own_v[:, part].astype(jnp.float32)
            own_ref[piece * per + h] = term.astype(own_ref.dtype)


def project_own(tokens, query, gain, w_uvqk, head):
    slots, width = tokens.shape
    heads = width // head
    pieces = 2
    whole = pl.BlockSpec(memory_space=pltpu.VMEM)
    return pl.pallas_call(
        functools.partial(own_kernel, head ** (-0.5), pieces),
        in_specs=[whole, whole, whole, pl.BlockSpec(memory_space=pltpu.HBM)],
        out_specs=[whole, whole],
        out_shape=[
            pltpu.VMEM((slots, width), jnp.bfloat16),
            pltpu.VMEM((heads, slots, head), jnp.bfloat16),
        ],
        scratch_shapes=[
            pltpu.VMEM((3, width, width), w_uvqk.dtype),
            pltpu.SemaphoreType.DMA((pieces, 3)),
        ],
        cost_estimate=pl.CostEstimate(
            flops=6 * slots * width * width, bytes_accessed=6 * width * width, transcendentals=3 * slots * width
        ),
        compiler_params=limit(14),
        name="project_own",
    )(tokens, query, gain.reshape(1, width), w_uvqk)


def visible_kernel(meta_ref, cache_ref, keys_ref, values_ref, sems):
    shards, length, head = keys_ref.shape
    visible = meta_ref[1]
    key_copy = pltpu.make_async_copy(cache_ref.at[:, 0], keys_ref, sems.at[0])
    value_copy = pltpu.make_async_copy(cache_ref.at[:, 1], values_ref, sems.at[1])
    key_copy.start()
    value_copy.start()
    key_copy.wait()
    for shard in range(shards):

        @pl.when(visible < (shard + 1) * length)
        def _():
            place = shard * length + lax.broadcasted_iota(jnp.int32, (length, head), 0)
            keys = keys_ref[shard].astype(jnp.float32)
            keys_ref[shard] = jnp.where(place < visible, keys, 0.0).astype(jnp.bfloat16)

    value_copy.wait()


def visible_prefix(meta, cache):
    shards, _, length, head = cache.shape
    kept = pltpu.VMEM((shards, length, head), cache.dtype)
    return pl.pallas_call(
        visible_kernel,
        in_specs=[pl.BlockSpec(memory_space=pltpu.SMEM), pl.BlockSpec(memory_space=pl.ANY)],
        out_specs=[pl.BlockSpec(memory_space=pltpu.VMEM), pl.BlockSpec(memory_space=pltpu.VMEM)],
        out_shape=[kept, kept],
        scratch_shapes=[pltpu.SemaphoreType.DMA((2,))],
        compiler_params=limit(1),
        name="visible_prefix",
    )(meta, cache)


def attend_kernel(scale, rows, chunk, groups, meta_ref, query_ref, keys_ref, values_ref, out_ref):
    blocks, slots, head = query_ref.shape
    shards, length, _ = keys_ref.shape
    per = rows // slots
    count = meta_ref[0]
    visible = meta_ref[1]
    live_blocks = jnp.minimum((count + rows - 1) // rows, blocks // per)

    def attend_to(used):
        span = used * length
        pieces = span // chunk

        def row_block(number, carry):
            first = number * per
            query = query_ref[pl.ds(first, per)].reshape(rows, head)
            query = (query.astype(jnp.float32) * (0.5 * scale)).astype(jnp.bfloat16)
            keys = keys_ref[:used].reshape(span, head)
            values = values_ref[:used].reshape(span, head)

            def scores(piece):
                part = keys[piece * chunk : (piece + 1) * chunk]
                return lax.dot_general(
                    query, part, (((1,), (1,)), ((), ())), preferred_element_type=jnp.float32
                )

            acc = jnp.zeros((rows, head), jnp.float32)
            ahead = scores(0)
            for piece in range(pieces):
                half = ahead.astype(jnp.bfloat16)
                if piece + 1 < pieces:
                    ahead = scores(piece + 1)
                weight = half + half * jnp.tanh(half)
                part = values[piece * chunk : (piece + 1) * chunk]
                acc = acc + jnp.dot(weight, part, preferred_element_type=jnp.float32)
            out_ref[pl.ds(first, per)] = acc.astype(jnp.bfloat16).reshape(per, slots, head)
            return carry

        lax.fori_loop(0, live_blocks, row_block, 0)

    below = 0
    for used in groups:
        within = visible > below * length
        if used < shards:
            within = jnp.logical_and(within, visible <= used * length)
        pl.when(within)(functools.partial(attend_to, used))
        below = used

    def dead_block(number, carry):
        out_ref[pl.ds(number * per, per)] = jnp.zeros((per, slots, head), jnp.bfloat16)
        return carry

    lax.fori_loop(live_blocks, blocks // per, dead_block, 0)


def attend(meta, query, keys, values):
    blocks, slots, head = query.shape
    shards, length, _ = keys.shape
    rows = 4 * slots
    groups = (shards // 2, shards)
    flops = 4 * blocks * slots * shards * length * head
    whole = pl.BlockSpec(memory_space=pltpu.VMEM)
    return pl.pallas_call(
        functools.partial(attend_kernel, head ** (-0.5), rows, length, groups),
        in_specs=[pl.BlockSpec(memory_space=pltpu.SMEM), whole, whole, whole],
        out_specs=whole,
        out_shape=jax.ShapeDtypeStruct(query.shape, jnp.bfloat16),
        cost_estimate=pl.CostEstimate(
            flops=flops, bytes_accessed=keys.size * 4, transcendentals=blocks * slots * shards * length
        ),
        compiler_params=limit(14),
        name="attend",
    )(meta, query, keys, values)


def finish_kernel(pieces, meta_ref, mixed_ref, own_ref, gate_ref, w_ref, out_ref):
    heads, slots, head = mixed_ref.shape
    count = meta_ref[0]
    first = meta_ref[2] * slots
    width = heads * head
    rows = slots // pieces
    for piece in range(pieces):
        here = slice(piece * rows, (piece + 1) * rows)
        mixed = jnp.concatenate(
            [
                mixed_ref[h, here].astype(jnp.float32) + own_ref[h, here].astype(jnp.float32)
                for h in range(heads)
            ],
            axis=1,
        )
        centre = mixed - jnp.sum(mixed, axis=-1, keepdims=True) * (1.0 / width)
        spread = jnp.sum(centre * centre, axis=-1, keepdims=True) * (1.0 / width)
        normed = centre * lax.rsqrt(spread + 1e-05) * gate_ref[here].astype(jnp.float32)
        result = jnp.dot(normed.astype(jnp.bfloat16), w_ref[...], preferred_element_type=jnp.float32)
        place = first + piece * rows + lax.broadcasted_iota(jnp.int32, result.shape, 0)
        out_ref[here] = jnp.where(place < count, result, 0.0).astype(jnp.bfloat16)


def finish(meta, mixed, own, gate, w_output):
    slots, width = gate.shape
    whole = pl.BlockSpec(memory_space=pltpu.VMEM)
    return pl.pallas_call(
        functools.partial(finish_kernel, 2),
        in_specs=[pl.BlockSpec(memory_space=pltpu.SMEM)] + [whole] * 4,
        out_specs=whole,
        out_shape=jax.ShapeDtypeStruct((slots, width), jnp.bfloat16),
        cost_estimate=pl.CostEstimate(
            flops=2 * slots * width * width, bytes_accessed=2 * width * width, transcendentals=slots
        ),
        compiler_params=limit(10),
        name="finish",
    )(meta, mixed, own, gate, w_output)


def local(candidates, prefix_cache, w_uvqk, w_output, norm_gain, owner, counts, prefix_len):
    groups = lax.axis_size("group")
    group_here = lax.axis_index("group")
    helper_here = lax.axis_index("helper")
    offset = jnp.minimum(lax.optimization_barrier(owner[0]), groups - 1)
    width = candidates.shape[2]
    head = width // HEADS
    near, far = route(offset, groups)
    nears = range(1 - FAR, FAR)
    fars = range(groups // FAR + 1)
    near_moves = [near_move(steps, groups, head) for steps in nears]
    far_moves = [far_move(FAR * steps, groups, head) for steps in fars]
    w_uvqk = pltpu.with_memory_space_constraint(w_uvqk, pltpu.HBM)
    prefix = pltpu.with_memory_space_constraint(prefix_cache[0], pltpu.HBM)
    tokens, split, w_query = lax.switch(near + FAR - 1, near_moves, candidates[0], prefix, w_uvqk)
    tokens, cache, query = lax.switch(far, far_moves, tokens, split, w_query)
    user = (group_here - offset) % groups
    table = jnp.stack([counts, prefix_len, jnp.full_like(counts, helper_here)])
    places = lax.broadcasted_iota(jnp.int32, table.shape, 1)
    meta = jnp.sum(jnp.where(places == user, table, 0), axis=1)
    query_all = exchange(query)
    gate, own = project_own(tokens, query, norm_gain, w_uvqk, head)
    keys, values = visible_prefix(meta, cache)
    heads_out = attend(meta, query_all, keys, values)
    mixed = exchange(heads_out)
    return finish(meta, mixed, own, gate, w_output)[None]


def solution(mesh):
    in_specs = (
        P("group", "helper", None),
        P("group", None, "helper", None),
        P(),
        P(),
        P(),
        P(),
        P(),
        P(),
    )
    out_specs = P("group", "helper", None)
    return jax.shard_map(local, mesh=mesh, in_specs=in_specs, out_specs=out_specs, check_vma=False)
```

```python
import functools

import jax
import jax.numpy as jnp
from jax import lax
from jax.experimental import pallas as pl
from jax.experimental.pallas import tpu as pltpu
from jax.sharding import PartitionSpec as P


HEADS = 8
FAR = 4


def silu(value):
    half = 0.5 * value
    return half + half * jnp.tanh(half)


def exchange(value):
    return lax.all_to_all(value, "helper", 0, 0, tiled=True)


def rotate(value, steps, count):
    if steps % count == 0:
        return value
    pairs = [(source, (source + steps) % count) for source in range(count)]
    return lax.ppermute(value, "group", pairs)


def first_move(steps, count, head):
    def move(tokens, cache, w_uvqk):
        if steps == 0:
            split, w_query, moved = prepare(cache, w_uvqk, head, tokens)
            return moved, split, w_query
        moved = rotate(tokens, steps, count)
        split, w_query = prepare(cache, w_uvqk, head)
        return moved, split, w_query

    return move


def second_move(steps, count, head):
    def move(tokens, split, w_query):
        moved = rotate(tokens, steps, count)
        cache = exchange(split)
        kept, query = project_query(moved, w_query, head)
        return kept, cache, query

    return move


def plan(groups):
    steps = []
    for offset in range(groups):
        signed = (offset + groups // 2 - 1) % groups - groups // 2 + 1
        size, sign = abs(signed), 1 if signed > 0 else -1
        if size < FAR:
            steps.append((0, signed))
            continue
        far = groups // 2 if size >= groups // 2 - FAR else size // FAR * FAR
        steps.append((sign * (size - far), sign * far if far < groups // 2 else far))
    firsts = sorted({first for first, _ in steps})
    seconds = sorted({second for _, second in steps})
    return firsts, seconds, [(firsts.index(x), seconds.index(y)) for x, y in steps]


def pick_int(values, index):
    runs = []
    at = 0
    while at < len(values):
        slope = values[at + 1] - values[at] if at + 1 < len(values) else 0
        end = at + 1
        while end < len(values) and values[end] - values[end - 1] == slope:
            end += 1
        runs.append((at, values[at], slope))
        at = end
    out = None
    for start, value, slope in runs:
        line = value + slope * (index - start) if slope else jnp.int32(value)
        out = line if out is None else jnp.where(index >= start, line, out)
    return out


def limit(mebibytes):
    return pltpu.CompilerParams(vmem_limit_bytes=mebibytes << 20)


def prepare(cache, w_uvqk, head, tokens=None):
    two, length, width = cache.shape
    heads = width // head
    shape = (heads, two, length, head)
    far = pl.BlockSpec(memory_space=pltpu.HBM)
    near = pl.BlockSpec(memory_space=pltpu.VMEM)

    def kernel(*refs):
        if tokens is None:
            cache_ref, w_ref, split_ref, query_ref, buf, reads, writes, sem = refs
        else:
            cache_ref, w_ref, tokens_ref, split_ref, query_ref, kept_ref, buf, reads, writes, sem, held, moves = refs
            pull_tokens = pltpu.make_async_copy(tokens_ref, held, moves.at[0])
            push_tokens = pltpu.make_async_copy(held, kept_ref, moves.at[1])

        def pull(h):
            cols = pl.ds(pl.multiple_of(h * head, head), head)
            return pltpu.make_async_copy(cache_ref.at[:, :, cols], buf.at[h], reads.at[h])

        def push(h):
            return pltpu.make_async_copy(buf.at[h], split_ref.at[h], writes.at[h])

        def each(step):
            def body(h, carry):
                step(h)
                return carry

            lax.fori_loop(0, heads, body, 0)

        def pass_on(h):
            pull(h).wait()
            push(h).start()

        weights = pltpu.make_async_copy(w_ref.at[:, 2 * width : 3 * width], query_ref, sem)
        if tokens is not None:
            pull_tokens.start()
        each(lambda h: pull(h).start())
        weights.start()
        if tokens is not None:
            pull_tokens.wait()
            push_tokens.start()
        each(pass_on)
        each(lambda h: push(h).wait())
        weights.wait()
        if tokens is not None:
            push_tokens.wait()

    operands = [cache, w_uvqk]
    out_specs = [far, near]
    out_shape = [pltpu.HBM(shape, cache.dtype), pltpu.VMEM((width, width), w_uvqk.dtype)]
    scratch = [
        pltpu.VMEM(shape, cache.dtype),
        pltpu.SemaphoreType.DMA((heads,)),
        pltpu.SemaphoreType.DMA((heads,)),
        pltpu.SemaphoreType.DMA,
    ]
    if tokens is not None:
        operands.append(tokens)
        out_specs.append(far)
        out_shape.append(pltpu.HBM(tokens.shape, tokens.dtype))
        scratch += [pltpu.VMEM(tokens.shape, tokens.dtype), pltpu.SemaphoreType.DMA((2,))]
    return pl.pallas_call(
        kernel,
        in_specs=[far] * len(operands),
        out_specs=out_specs,
        out_shape=out_shape,
        scratch_shapes=scratch,
        compiler_params=limit(4),
        name="prepare",
    )(*operands)


def query_kernel(tokens_ref, w_ref, kept_ref, out_ref, sem):
    heads, _, head = out_ref.shape
    keep = pltpu.make_async_copy(tokens_ref, kept_ref, sem)
    keep.start()
    tokens = tokens_ref[...]
    per = heads // 2

    def some_heads(part, carry):
        cols = pl.ds(pl.multiple_of(part * per * head, head), per * head)
        proj = jnp.dot(tokens, w_ref[:, cols], preferred_element_type=jnp.float32)
        proj = silu(proj).astype(jnp.bfloat16)
        for h in range(per):
            out_ref[part * per + h] = proj[:, h * head : (h + 1) * head]
        return carry

    lax.fori_loop(0, 2, some_heads, 0)
    keep.wait()


def project_query(tokens, w_query, head):
    slots, width = tokens.shape
    heads = width // head
    whole = pl.BlockSpec(memory_space=pltpu.VMEM)
    return pl.pallas_call(
        query_kernel,
        in_specs=[whole, whole],
        out_specs=[pl.BlockSpec(memory_space=pltpu.HBM), whole],
        out_shape=[
            pltpu.HBM(tokens.shape, tokens.dtype),
            jax.ShapeDtypeStruct((heads, slots, head), jnp.bfloat16),
        ],
        scratch_shapes=[pltpu.SemaphoreType.DMA],
        cost_estimate=pl.CostEstimate(
            flops=2 * slots * width * width, bytes_accessed=2 * width * width, transcendentals=slots * width
        ),
        compiler_params=limit(8),
        name="project_query",
    )(tokens, w_query)


def own_kernel(scale, pieces, tokens_ref, query_ref, gain_ref, w_ref, gate_ref, own_ref, weights, sems):
    heads, _, head = query_ref.shape
    width = heads * head
    cols = width // pieces
    per = cols // head
    places = (0, 1, 3)

    def pull(piece, part):
        first = places[part] * width + piece * cols
        return pltpu.make_async_copy(
            w_ref.at[:, first : first + cols],
            weights.at[part, :, piece * cols : (piece + 1) * cols],
            sems.at[piece, part],
        )

    for piece in range(pieces):
        for part in (1, 2, 0):
            pull(piece, part).start()
    tokens = tokens_ref[...]

    def project(piece, part):
        pull(piece, part).wait()
        here = weights[part, :, piece * cols : (piece + 1) * cols]
        return silu(jnp.dot(tokens, here, preferred_element_type=jnp.float32))

    for piece in range(pieces):
        here = slice(piece * cols, (piece + 1) * cols)
        own_v = project(piece, 1).astype(jnp.bfloat16)
        own_k = project(piece, 2).astype(jnp.bfloat16)
        gate_ref[:, here] = (project(piece, 0) * gain_ref[:, here]).astype(gate_ref.dtype)
        for h in range(per):
            part = slice(h * head, (h + 1) * head)
            query = query_ref[piece * per + h].astype(jnp.float32)
            score = jnp.sum(query * own_k[:, part].astype(jnp.float32), axis=-1, keepdims=True) * scale
            weight = silu(score).astype(jnp.bfloat16).astype(jnp.float32)
            term = weight * own_v[:, part].astype(jnp.float32)
            own_ref[piece * per + h] = term.astype(own_ref.dtype)


def project_own(tokens, query, gain, w_uvqk, head):
    slots, width = tokens.shape
    heads = width // head
    pieces = 2
    whole = pl.BlockSpec(memory_space=pltpu.VMEM)
    return pl.pallas_call(
        functools.partial(own_kernel, head ** (-0.5), pieces),
        in_specs=[whole, whole, whole, pl.BlockSpec(memory_space=pltpu.HBM)],
        out_specs=[whole, whole],
        out_shape=[
            pltpu.VMEM((slots, width), jnp.bfloat16),
            pltpu.VMEM((heads, slots, head), jnp.bfloat16),
        ],
        scratch_shapes=[
            pltpu.VMEM((3, width, width), w_uvqk.dtype),
            pltpu.SemaphoreType.DMA((pieces, 3)),
        ],
        cost_estimate=pl.CostEstimate(
            flops=6 * slots * width * width, bytes_accessed=6 * width * width, transcendentals=3 * slots * width
        ),
        compiler_params=limit(14),
        name="project_own",
    )(tokens, query, gain.reshape(1, width), w_uvqk)


def visible_kernel(meta_ref, cache_ref, keys_ref, values_ref, sems):
    shards, length, head = keys_ref.shape
    visible = meta_ref[1]
    key_copy = pltpu.make_async_copy(cache_ref.at[:, 0], keys_ref, sems.at[0])
    value_copy = pltpu.make_async_copy(cache_ref.at[:, 1], values_ref, sems.at[1])
    key_copy.start()
    value_copy.start()
    key_copy.wait()
    for shard in range(shards):

        @pl.when(visible < (shard + 1) * length)
        def _():
            place = shard * length + lax.broadcasted_iota(jnp.int32, (length, head), 0)
            keys = keys_ref[shard].astype(jnp.float32)
            keys_ref[shard] = jnp.where(place < visible, keys, 0.0).astype(jnp.bfloat16)

    value_copy.wait()


def visible_prefix(meta, cache):
    shards, _, length, head = cache.shape
    kept = pltpu.VMEM((shards, length, head), cache.dtype)
    return pl.pallas_call(
        visible_kernel,
        in_specs=[pl.BlockSpec(memory_space=pltpu.SMEM), pl.BlockSpec(memory_space=pl.ANY)],
        out_specs=[pl.BlockSpec(memory_space=pltpu.VMEM), pl.BlockSpec(memory_space=pltpu.VMEM)],
        out_shape=[kept, kept],
        scratch_shapes=[pltpu.SemaphoreType.DMA((2,))],
        compiler_params=limit(1),
        name="visible_prefix",
    )(meta, cache)


def attend_kernel(scale, rows, meta_ref, query_ref, keys_ref, values_ref, out_ref):
    blocks, slots, head = query_ref.shape
    shards, _, _ = keys_ref.shape
    per = rows // slots
    live_blocks = jnp.minimum((meta_ref[0] + rows - 1) // rows, blocks // per)

    def row_block(number, carry):
        first = number * per
        query = query_ref[pl.ds(first, per)].reshape(rows, head)
        query = (query.astype(jnp.float32) * (0.5 * scale)).astype(jnp.bfloat16)

        def scores(shard):
            return lax.dot_general(
                query, keys_ref[shard], (((1,), (1,)), ((), ())), preferred_element_type=jnp.float32
            )

        acc = jnp.zeros((rows, head), jnp.float32)
        ahead = scores(0)
        for shard in range(shards):
            half = ahead.astype(jnp.bfloat16)
            if shard + 1 < shards:
                ahead = scores(shard + 1)
            weight = half + half * jnp.tanh(half)
            acc = acc + jnp.dot(weight, values_ref[shard], preferred_element_type=jnp.float32)
        out_ref[pl.ds(first, per)] = acc.astype(jnp.bfloat16).reshape(per, slots, head)
        return carry

    lax.fori_loop(0, live_blocks, row_block, 0)

    def dead_block(number, carry):
        out_ref[pl.ds(number * per, per)] = jnp.zeros((per, slots, head), jnp.bfloat16)
        return carry

    lax.fori_loop(live_blocks, blocks // per, dead_block, 0)


def attend(meta, query, keys, values):
    blocks, slots, head = query.shape
    shards, length, _ = keys.shape
    rows = 4 * slots
    flops = 4 * blocks * slots * shards * length * head
    whole = pl.BlockSpec(memory_space=pltpu.VMEM)
    return pl.pallas_call(
        functools.partial(attend_kernel, head ** (-0.5), rows),
        in_specs=[pl.BlockSpec(memory_space=pltpu.SMEM), whole, whole, whole],
        out_specs=whole,
        out_shape=jax.ShapeDtypeStruct(query.shape, jnp.bfloat16),
        cost_estimate=pl.CostEstimate(
            flops=flops, bytes_accessed=keys.size * 4, transcendentals=blocks * slots * shards * length
        ),
        compiler_params=limit(14),
        name="attend",
    )(meta, query, keys, values)


def finish_kernel(pieces, meta_ref, mixed_ref, own_ref, gate_ref, w_ref, out_ref, buf, sems):
    heads, slots, head = mixed_ref.shape
    count = meta_ref[0]
    first = meta_ref[2] * slots
    width = heads * head
    rows = slots // pieces
    copies = []
    for piece in range(pieces):
        here = slice(piece * rows, (piece + 1) * rows)
        mixed = jnp.concatenate(
            [
                mixed_ref[h, here].astype(jnp.float32) + own_ref[h, here].astype(jnp.float32)
                for h in range(heads)
            ],
            axis=1,
        )
        centre = mixed - jnp.sum(mixed, axis=-1, keepdims=True) * (1.0 / width)
        spread = jnp.sum(centre * centre, axis=-1, keepdims=True) * (1.0 / width)
        normed = centre * lax.rsqrt(spread + 1e-05) * gate_ref[here].astype(jnp.float32)
        result = jnp.dot(normed.astype(jnp.bfloat16), w_ref[...], preferred_element_type=jnp.float32)
        place = first + piece * rows + lax.broadcasted_iota(jnp.int32, result.shape, 0)
        buf[here] = jnp.where(place < count, result, 0.0).astype(jnp.bfloat16)
        copies.append(pltpu.make_async_copy(buf.at[here], out_ref.at[here], sems.at[piece]))
        copies[-1].start()
    for copy in copies:
        copy.wait()


def finish(meta, mixed, own, gate, w_output):
    slots, width = gate.shape
    pieces = 2
    whole = pl.BlockSpec(memory_space=pltpu.VMEM)
    return pl.pallas_call(
        functools.partial(finish_kernel, pieces),
        in_specs=[pl.BlockSpec(memory_space=pltpu.SMEM)] + [whole] * 4,
        out_specs=pl.BlockSpec(memory_space=pltpu.HBM),
        scratch_shapes=[pltpu.VMEM((slots, width), jnp.bfloat16), pltpu.SemaphoreType.DMA((pieces,))],
        out_shape=jax.ShapeDtypeStruct((slots, width), jnp.bfloat16),
        cost_estimate=pl.CostEstimate(
            flops=2 * slots * width * width, bytes_accessed=2 * width * width, transcendentals=slots
        ),
        compiler_params=limit(10),
        name="finish",
    )(meta, mixed, own, gate, w_output)


def local(candidates, prefix_cache, w_uvqk, w_output, norm_gain, owner, counts, prefix_len):
    groups = lax.axis_size("group")
    group_here = lax.axis_index("group")
    helper_here = lax.axis_index("helper")
    offset = jnp.minimum(lax.optimization_barrier(owner[0]), groups - 1)
    width = candidates.shape[2]
    head = width // HEADS
    firsts, seconds, steps = plan(groups)
    first = pick_int([x for x, _ in steps], offset)
    second = pick_int([y for _, y in steps], offset)
    first_moves = [first_move(by, groups, head) for by in firsts]
    second_moves = [second_move(by, groups, head) for by in seconds]
    w_uvqk = pltpu.with_memory_space_constraint(w_uvqk, pltpu.HBM)
    prefix = pltpu.with_memory_space_constraint(prefix_cache[0], pltpu.HBM)
    tokens, split, w_query = lax.switch(first, first_moves, candidates[0], prefix, w_uvqk)
    tokens, cache, query = lax.switch(second, second_moves, tokens, split, w_query)
    user = (group_here - offset) % groups
    table = jnp.stack([counts, prefix_len, jnp.full_like(counts, helper_here)])
    places = lax.broadcasted_iota(jnp.int32, table.shape, 1)
    meta = jnp.sum(jnp.where(places == user, table, 0), axis=1)
    query_all = exchange(query)
    gate, own = project_own(tokens, query, norm_gain, w_uvqk, head)
    keys, values = visible_prefix(meta, cache)
    heads_out = attend(meta, query_all, keys, values)
    mixed = exchange(heads_out)
    return finish(meta, mixed, own, gate, w_output)[None]


def solution(mesh):
    in_specs = (
        P("group", "helper", None),
        P("group", None, "helper", None),
        P(),
        P(),
        P(),
        P(),
        P(),
        P(),
    )
    out_specs = P("group", "helper", None)
    return jax.shard_map(local, mesh=mesh, in_specs=in_specs, out_specs=out_specs, check_vma=False)
```

```python
import functools

import jax
import jax.numpy as jnp
from jax import lax
from jax.experimental import pallas as pl
from jax.experimental.pallas import tpu as pltpu
from jax.sharding import PartitionSpec as P


HEADS = 8
FAR = 4


def silu(value):
    half = 0.5 * value
    return half + half * jnp.tanh(half)


def exchange(value):
    return lax.all_to_all(value, "helper", 0, 0, tiled=True)


def rotate(value, steps, count):
    if steps % count == 0:
        return value
    pairs = [(source, (source + steps) % count) for source in range(count)]
    return lax.ppermute(value, "group", pairs)


def first_move(steps, count, head):
    def move(tokens, cache):
        if steps == 0:
            split, moved = prepare(cache, head, tokens)
            return moved, split
        moved = rotate(tokens, steps, count)
        (split,) = prepare(cache, head)
        return moved, split

    return move


def second_move(steps, count, head):
    def move(tokens, split, w_uvqk):
        moved = rotate(tokens, steps, count)
        cache = exchange(split)
        w_query = fetch(w_uvqk)
        kept, query = project_query(moved, w_query, head)
        return kept, cache, query

    return move


def plan(groups):
    steps = []
    for offset in range(groups):
        signed = (offset + groups // 2 - 1) % groups - groups // 2 + 1
        size, sign = abs(signed), 1 if signed > 0 else -1
        if size < FAR:
            steps.append((0, signed))
            continue
        far = groups // 2 if size >= groups // 2 - FAR else size // FAR * FAR
        steps.append((sign * (size - far), sign * far if far < groups // 2 else far))
    firsts = sorted({first for first, _ in steps})
    seconds = sorted({second for _, second in steps})
    return firsts, seconds, [(firsts.index(x), seconds.index(y)) for x, y in steps]


def pick_int(values, index):
    runs = []
    at = 0
    while at < len(values):
        slope = values[at + 1] - values[at] if at + 1 < len(values) else 0
        end = at + 1
        while end < len(values) and values[end] - values[end - 1] == slope:
            end += 1
        runs.append((at, values[at], slope))
        at = end
    out = None
    for start, value, slope in runs:
        line = value + slope * (index - start) if slope else jnp.int32(value)
        out = line if out is None else jnp.where(index >= start, line, out)
    return out


def limit(mebibytes):
    return pltpu.CompilerParams(vmem_limit_bytes=mebibytes << 20)


def prepare(cache, head, tokens=None):
    two, length, width = cache.shape
    heads = width // head
    shape = (heads, two, length, head)
    far = pl.BlockSpec(memory_space=pltpu.HBM)

    def kernel(*refs):
        if tokens is None:
            cache_ref, split_ref, buf, reads, writes = refs
        else:
            cache_ref, tokens_ref, split_ref, kept_ref, buf, reads, writes, held, moves = refs
            pull_tokens = pltpu.make_async_copy(tokens_ref, held, moves.at[0])
            push_tokens = pltpu.make_async_copy(held, kept_ref, moves.at[1])

        def pull(h):
            cols = pl.ds(pl.multiple_of(h * head, head), head)
            return pltpu.make_async_copy(cache_ref.at[:, :, cols], buf.at[h], reads.at[h])

        def push(h):
            return pltpu.make_async_copy(buf.at[h], split_ref.at[h], writes.at[h])

        def each(step):
            def body(h, carry):
                step(h)
                return carry

            lax.fori_loop(0, heads, body, 0)

        def pass_on(h):
            pull(h).wait()
            push(h).start()

        if tokens is not None:
            pull_tokens.start()
        each(lambda h: pull(h).start())
        if tokens is not None:
            pull_tokens.wait()
            push_tokens.start()
        each(pass_on)
        each(lambda h: push(h).wait())
        if tokens is not None:
            push_tokens.wait()

    operands = [cache]
    out_specs = [far]
    out_shape = [pltpu.HBM(shape, cache.dtype)]
    scratch = [
        pltpu.VMEM(shape, cache.dtype),
        pltpu.SemaphoreType.DMA((heads,)),
        pltpu.SemaphoreType.DMA((heads,)),
    ]
    if tokens is not None:
        operands.append(tokens)
        out_specs.append(far)
        out_shape.append(pltpu.HBM(tokens.shape, tokens.dtype))
        scratch += [pltpu.VMEM(tokens.shape, tokens.dtype), pltpu.SemaphoreType.DMA((2,))]
    return pl.pallas_call(
        kernel,
        in_specs=[far] * len(operands),
        out_specs=out_specs,
        out_shape=out_shape,
        scratch_shapes=scratch,
        compiler_params=limit(4),
        name="prepare",
    )(*operands)


def fetch_kernel(w_uvqk_ref, query_ref, sem):
    width = query_ref.shape[1]
    copy = pltpu.make_async_copy(w_uvqk_ref.at[:, 2 * width : 3 * width], query_ref, sem)
    copy.start()
    copy.wait()


def fetch(w_uvqk):
    width = w_uvqk.shape[0]
    return pl.pallas_call(
        fetch_kernel,
        in_specs=[pl.BlockSpec(memory_space=pltpu.HBM)],
        out_specs=pl.BlockSpec(memory_space=pltpu.VMEM),
        out_shape=pltpu.VMEM((width, width), w_uvqk.dtype),
        scratch_shapes=[pltpu.SemaphoreType.DMA],
        compiler_params=limit(1),
        name="fetch",
    )(w_uvqk)


def query_kernel(tokens_ref, w_ref, kept_ref, out_ref, sem):
    heads, _, head = out_ref.shape
    keep = pltpu.make_async_copy(tokens_ref, kept_ref, sem)
    keep.start()
    tokens = tokens_ref[...]
    per = heads // 2

    def some_heads(part, carry):
        cols = pl.ds(pl.multiple_of(part * per * head, head), per * head)
        proj = jnp.dot(tokens, w_ref[:, cols], preferred_element_type=jnp.float32)
        proj = silu(proj).astype(jnp.bfloat16)
        for h in range(per):
            out_ref[part * per + h] = proj[:, h * head : (h + 1) * head]
        return carry

    lax.fori_loop(0, 2, some_heads, 0)
    keep.wait()


def project_query(tokens, w_query, head):
    slots, width = tokens.shape
    heads = width // head
    whole = pl.BlockSpec(memory_space=pltpu.VMEM)
    return pl.pallas_call(
        query_kernel,
        in_specs=[whole, whole],
        out_specs=[pl.BlockSpec(memory_space=pltpu.HBM), whole],
        out_shape=[
            pltpu.HBM(tokens.shape, tokens.dtype),
            jax.ShapeDtypeStruct((heads, slots, head), jnp.bfloat16),
        ],
        scratch_shapes=[pltpu.SemaphoreType.DMA],
        cost_estimate=pl.CostEstimate(
            flops=2 * slots * width * width, bytes_accessed=2 * width * width, transcendentals=slots * width
        ),
        compiler_params=limit(8),
        name="project_query",
    )(tokens, w_query)


def own_kernel(scale, pieces, tokens_ref, query_ref, gain_ref, w_ref, gate_ref, own_ref, weights, sems):
    heads, _, head = query_ref.shape
    width = heads * head
    cols = width // pieces
    per = cols // head
    places = (0, 1, 3)

    def pull(piece, part):
        first = places[part] * width + piece * cols
        return pltpu.make_async_copy(
            w_ref.at[:, first : first + cols],
            weights.at[part, :, piece * cols : (piece + 1) * cols],
            sems.at[piece, part],
        )

    for piece in range(pieces):
        for part in (1, 2, 0):
            pull(piece, part).start()
    tokens = tokens_ref[...]

    def project(piece, part):
        pull(piece, part).wait()
        here = weights[part, :, piece * cols : (piece + 1) * cols]
        return silu(jnp.dot(tokens, here, preferred_element_type=jnp.float32))

    for piece in range(pieces):
        here = slice(piece * cols, (piece + 1) * cols)
        own_v = project(piece, 1).astype(jnp.bfloat16)
        own_k = project(piece, 2).astype(jnp.bfloat16)
        gate_ref[:, here] = (project(piece, 0) * gain_ref[:, here]).astype(gate_ref.dtype)
        for h in range(per):
            part = slice(h * head, (h + 1) * head)
            query = query_ref[piece * per + h].astype(jnp.float32)
            score = jnp.sum(query * own_k[:, part].astype(jnp.float32), axis=-1, keepdims=True) * scale
            weight = silu(score).astype(jnp.bfloat16).astype(jnp.float32)
            term = weight * own_v[:, part].astype(jnp.float32)
            own_ref[piece * per + h] = term.astype(own_ref.dtype)


def project_own(tokens, query, gain, w_uvqk, head):
    slots, width = tokens.shape
    heads = width // head
    pieces = 2
    whole = pl.BlockSpec(memory_space=pltpu.VMEM)
    return pl.pallas_call(
        functools.partial(own_kernel, head ** (-0.5), pieces),
        in_specs=[whole, whole, whole, pl.BlockSpec(memory_space=pltpu.HBM)],
        out_specs=[whole, whole],
        out_shape=[
            pltpu.VMEM((slots, width), jnp.bfloat16),
            pltpu.VMEM((heads, slots, head), jnp.bfloat16),
        ],
        scratch_shapes=[
            pltpu.VMEM((3, width, width), w_uvqk.dtype),
            pltpu.SemaphoreType.DMA((pieces, 3)),
        ],
        cost_estimate=pl.CostEstimate(
            flops=6 * slots * width * width, bytes_accessed=6 * width * width, transcendentals=3 * slots * width
        ),
        compiler_params=limit(14),
        name="project_own",
    )(tokens, query, gain.reshape(1, width), w_uvqk)


def visible_kernel(meta_ref, cache_ref, keys_ref, values_ref, sems):
    shards, length, head = keys_ref.shape
    visible = meta_ref[1]
    key_copy = pltpu.make_async_copy(cache_ref.at[:, 0], keys_ref, sems.at[0])
    value_copy = pltpu.make_async_copy(cache_ref.at[:, 1], values_ref, sems.at[1])
    key_copy.start()
    value_copy.start()
    key_copy.wait()
    for shard in range(shards):

        @pl.when(visible < (shard + 1) * length)
        def _():
            place = shard * length + lax.broadcasted_iota(jnp.int32, (length, head), 0)
            keys = keys_ref[shard].astype(jnp.float32)
            keys_ref[shard] = jnp.where(place < visible, keys, 0.0).astype(jnp.bfloat16)

    value_copy.wait()


def visible_prefix(meta, cache):
    shards, _, length, head = cache.shape
    kept = pltpu.VMEM((shards, length, head), cache.dtype)
    return pl.pallas_call(
        visible_kernel,
        in_specs=[pl.BlockSpec(memory_space=pltpu.SMEM), pl.BlockSpec(memory_space=pl.ANY)],
        out_specs=[pl.BlockSpec(memory_space=pltpu.VMEM), pl.BlockSpec(memory_space=pltpu.VMEM)],
        out_shape=[kept, kept],
        scratch_shapes=[pltpu.SemaphoreType.DMA((2,))],
        compiler_params=limit(1),
        name="visible_prefix",
    )(meta, cache)


def attend_kernel(scale, rows, meta_ref, query_ref, keys_ref, values_ref, out_ref):
    blocks, slots, head = query_ref.shape
    shards, _, _ = keys_ref.shape
    per = rows // slots
    live_blocks = jnp.minimum((meta_ref[0] + rows - 1) // rows, blocks // per)

    def row_block(number, carry):
        first = number * per
        query = query_ref[pl.ds(first, per)].reshape(rows, head)
        query = (query.astype(jnp.float32) * (0.5 * scale)).astype(jnp.bfloat16)

        def scores(shard):
            return lax.dot_general(
                query, keys_ref[shard], (((1,), (1,)), ((), ())), preferred_element_type=jnp.float32
            )

        acc = jnp.zeros((rows, head), jnp.float32)
        ahead = scores(0)
        for shard in range(shards):
            half = ahead.astype(jnp.bfloat16)
            if shard + 1 < shards:
                ahead = scores(shard + 1)
            weight = half + half * jnp.tanh(half)
            acc = acc + jnp.dot(weight, values_ref[shard], preferred_element_type=jnp.float32)
        out_ref[pl.ds(first, per)] = acc.astype(jnp.bfloat16).reshape(per, slots, head)
        return carry

    lax.fori_loop(0, live_blocks, row_block, 0)

    def dead_block(number, carry):
        out_ref[pl.ds(number * per, per)] = jnp.zeros((per, slots, head), jnp.bfloat16)
        return carry

    lax.fori_loop(live_blocks, blocks // per, dead_block, 0)


def attend(meta, query, keys, values):
    blocks, slots, head = query.shape
    shards, length, _ = keys.shape
    rows = 4 * slots
    flops = 4 * blocks * slots * shards * length * head
    whole = pl.BlockSpec(memory_space=pltpu.VMEM)
    return pl.pallas_call(
        functools.partial(attend_kernel, head ** (-0.5), rows),
        in_specs=[pl.BlockSpec(memory_space=pltpu.SMEM), whole, whole, whole],
        out_specs=whole,
        out_shape=jax.ShapeDtypeStruct(query.shape, jnp.bfloat16),
        cost_estimate=pl.CostEstimate(
            flops=flops, bytes_accessed=keys.size * 4, transcendentals=blocks * slots * shards * length
        ),
        compiler_params=limit(14),
        name="attend",
    )(meta, query, keys, values)


def finish_kernel(pieces, meta_ref, mixed_ref, own_ref, gate_ref, w_ref, out_ref, buf, sems):
    heads, slots, head = mixed_ref.shape
    count = meta_ref[0]
    first = meta_ref[2] * slots
    width = heads * head
    rows = slots // pieces
    copies = []
    for piece in range(pieces):
        here = slice(piece * rows, (piece + 1) * rows)
        mixed = jnp.concatenate(
            [
                mixed_ref[h, here].astype(jnp.float32) + own_ref[h, here].astype(jnp.float32)
                for h in range(heads)
            ],
            axis=1,
        )
        centre = mixed - jnp.sum(mixed, axis=-1, keepdims=True) * (1.0 / width)
        spread = jnp.sum(centre * centre, axis=-1, keepdims=True) * (1.0 / width)
        normed = centre * lax.rsqrt(spread + 1e-05) * gate_ref[here].astype(jnp.float32)
        result = jnp.dot(normed.astype(jnp.bfloat16), w_ref[...], preferred_element_type=jnp.float32)
        place = first + piece * rows + lax.broadcasted_iota(jnp.int32, result.shape, 0)
        buf[here] = jnp.where(place < count, result, 0.0).astype(jnp.bfloat16)
        copies.append(pltpu.make_async_copy(buf.at[here], out_ref.at[here], sems.at[piece]))
        copies[-1].start()
    for copy in copies:
        copy.wait()


def finish(meta, mixed, own, gate, w_output):
    slots, width = gate.shape
    pieces = 2
    whole = pl.BlockSpec(memory_space=pltpu.VMEM)
    return pl.pallas_call(
        functools.partial(finish_kernel, pieces),
        in_specs=[pl.BlockSpec(memory_space=pltpu.SMEM)] + [whole] * 4,
        out_specs=pl.BlockSpec(memory_space=pltpu.HBM),
        scratch_shapes=[pltpu.VMEM((slots, width), jnp.bfloat16), pltpu.SemaphoreType.DMA((pieces,))],
        out_shape=jax.ShapeDtypeStruct((slots, width), jnp.bfloat16),
        cost_estimate=pl.CostEstimate(
            flops=2 * slots * width * width, bytes_accessed=2 * width * width, transcendentals=slots
        ),
        compiler_params=limit(10),
        name="finish",
    )(meta, mixed, own, gate, w_output)


def local(candidates, prefix_cache, w_uvqk, w_output, norm_gain, owner, counts, prefix_len):
    groups = lax.axis_size("group")
    group_here = lax.axis_index("group")
    helper_here = lax.axis_index("helper")
    offset = jnp.minimum(lax.optimization_barrier(owner[0]), groups - 1)
    width = candidates.shape[2]
    head = width // HEADS
    firsts, seconds, steps = plan(groups)
    first = pick_int([x for x, _ in steps], offset)
    second = pick_int([y for _, y in steps], offset)
    first_moves = [first_move(by, groups, head) for by in firsts]
    second_moves = [second_move(by, groups, head) for by in seconds]
    w_uvqk = pltpu.with_memory_space_constraint(w_uvqk, pltpu.HBM)
    prefix = pltpu.with_memory_space_constraint(prefix_cache[0], pltpu.HBM)
    tokens, split = lax.switch(first, first_moves, candidates[0], prefix)
    tokens, cache, query = lax.switch(second, second_moves, tokens, split, w_uvqk)
    user = (group_here - offset) % groups
    table = jnp.stack([counts, prefix_len, jnp.full_like(counts, helper_here)])
    places = lax.broadcasted_iota(jnp.int32, table.shape, 1)
    meta = jnp.sum(jnp.where(places == user, table, 0), axis=1)
    query_all = exchange(query)
    gate, own = project_own(tokens, query, norm_gain, w_uvqk, head)
    keys, values = visible_prefix(meta, cache)
    heads_out = attend(meta, query_all, keys, values)
    mixed = exchange(heads_out)
    return finish(meta, mixed, own, gate, w_output)[None]


def solution(mesh):
    in_specs = (
        P("group", "helper", None),
        P("group", None, "helper", None),
        P(),
        P(),
        P(),
        P(),
        P(),
        P(),
    )
    out_specs = P("group", "helper", None)
    return jax.shard_map(local, mesh=mesh, in_specs=in_specs, out_specs=out_specs, check_vma=False)
```

```python
import functools

import jax
import jax.numpy as jnp
from jax import lax
from jax.experimental import pallas as pl
from jax.experimental.pallas import tpu as pltpu
from jax.sharding import PartitionSpec as P


HEADS = 8
FAR = 4


def silu(value):
    half = 0.5 * value
    return half + half * jnp.tanh(half)


def exchange(value):
    return lax.all_to_all(value, "helper", 0, 0, tiled=True)


def rotate(value, steps, count):
    if steps % count == 0:
        return value
    pairs = [(source, (source + steps) % count) for source in range(count)]
    return lax.ppermute(value, "group", pairs)


def first_move(steps, count, head):
    def move(tokens, cache):
        if steps == 0:
            split, moved = prepare(cache, head, tokens)
            return moved, split
        moved = rotate(tokens, steps, count)
        (split,) = prepare(cache, head)
        return moved, split

    return move


def second_move(steps, count, head):
    def move(tokens, split, w_uvqk):
        moved = rotate(tokens, steps, count)
        cache = exchange(split)
        w_query = fetch(w_uvqk)
        kept, query = project_query(moved, w_query, head)
        return kept, cache, query

    return move


def plan(groups):
    steps = []
    for offset in range(groups):
        signed = (offset + groups // 2 - 1) % groups - groups // 2 + 1
        size, sign = abs(signed), 1 if signed > 0 else -1
        if size < FAR:
            steps.append((0, signed))
            continue
        far = groups // 2 if size >= groups // 2 - FAR else size // FAR * FAR
        steps.append((sign * (size - far), sign * far if far < groups // 2 else far))
    firsts = sorted({first for first, _ in steps})
    seconds = sorted({second for _, second in steps})
    return firsts, seconds, [(firsts.index(x), seconds.index(y)) for x, y in steps]


def pick_int(values, index):
    runs = []
    at = 0
    while at < len(values):
        slope = values[at + 1] - values[at] if at + 1 < len(values) else 0
        end = at + 1
        while end < len(values) and values[end] - values[end - 1] == slope:
            end += 1
        runs.append((at, values[at], slope))
        at = end
    out = None
    for start, value, slope in runs:
        line = value + slope * (index - start) if slope else jnp.int32(value)
        out = line if out is None else jnp.where(index >= start, line, out)
    return out


def limit(mebibytes):
    return pltpu.CompilerParams(vmem_limit_bytes=mebibytes << 20)


def prepare(cache, head, tokens=None):
    two, length, width = cache.shape
    heads = width // head
    shape = (heads, two, length, head)
    far = pl.BlockSpec(memory_space=pltpu.HBM)

    def kernel(*refs):
        if tokens is None:
            cache_ref, split_ref, buf, reads, writes = refs
        else:
            cache_ref, tokens_ref, split_ref, kept_ref, buf, reads, writes, held, moves = refs
            pull_tokens = pltpu.make_async_copy(tokens_ref, held, moves.at[0])
            push_tokens = pltpu.make_async_copy(held, kept_ref, moves.at[1])

        def pull(h):
            cols = pl.ds(pl.multiple_of(h * head, head), head)
            return pltpu.make_async_copy(cache_ref.at[:, :, cols], buf.at[h], reads.at[h])

        def push(h):
            return pltpu.make_async_copy(buf.at[h], split_ref.at[h], writes.at[h])

        def each(step):
            def body(h, carry):
                step(h)
                return carry

            lax.fori_loop(0, heads, body, 0)

        def pass_on(h):
            pull(h).wait()
            push(h).start()

        if tokens is not None:
            pull_tokens.start()
        each(lambda h: pull(h).start())
        if tokens is not None:
            pull_tokens.wait()
            push_tokens.start()
        each(pass_on)
        each(lambda h: push(h).wait())
        if tokens is not None:
            push_tokens.wait()

    operands = [cache]
    out_specs = [far]
    out_shape = [pltpu.HBM(shape, cache.dtype)]
    scratch = [
        pltpu.VMEM(shape, cache.dtype),
        pltpu.SemaphoreType.DMA((heads,)),
        pltpu.SemaphoreType.DMA((heads,)),
    ]
    if tokens is not None:
        operands.append(tokens)
        out_specs.append(far)
        out_shape.append(pltpu.HBM(tokens.shape, tokens.dtype))
        scratch += [pltpu.VMEM(tokens.shape, tokens.dtype), pltpu.SemaphoreType.DMA((2,))]
    return pl.pallas_call(
        kernel,
        in_specs=[far] * len(operands),
        out_specs=out_specs,
        out_shape=out_shape,
        scratch_shapes=scratch,
        compiler_params=limit(4),
        name="prepare",
    )(*operands)


def fetch_kernel(w_uvqk_ref, query_ref, sem):
    width = query_ref.shape[1]
    copy = pltpu.make_async_copy(w_uvqk_ref.at[:, 2 * width : 3 * width], query_ref, sem)
    copy.start()
    copy.wait()


def fetch(w_uvqk):
    width = w_uvqk.shape[0]
    return pl.pallas_call(
        fetch_kernel,
        in_specs=[pl.BlockSpec(memory_space=pltpu.HBM)],
        out_specs=pl.BlockSpec(memory_space=pltpu.VMEM),
        out_shape=pltpu.VMEM((width, width), w_uvqk.dtype),
        scratch_shapes=[pltpu.SemaphoreType.DMA],
        compiler_params=limit(1),
        name="fetch",
    )(w_uvqk)


def query_kernel(tokens_ref, w_ref, kept_ref, out_ref, sem):
    heads, _, head = out_ref.shape
    keep = pltpu.make_async_copy(tokens_ref, kept_ref, sem)
    keep.start()
    tokens = tokens_ref[...]
    per = heads // 2

    def some_heads(part, carry):
        cols = pl.ds(pl.multiple_of(part * per * head, head), per * head)
        proj = jnp.dot(tokens, w_ref[:, cols], preferred_element_type=jnp.float32)
        proj = silu(proj).astype(jnp.bfloat16)
        for h in range(per):
            out_ref[part * per + h] = proj[:, h * head : (h + 1) * head]
        return carry

    lax.fori_loop(0, 2, some_heads, 0)
    keep.wait()


def project_query(tokens, w_query, head):
    slots, width = tokens.shape
    heads = width // head
    whole = pl.BlockSpec(memory_space=pltpu.VMEM)
    return pl.pallas_call(
        query_kernel,
        in_specs=[whole, whole],
        out_specs=[pl.BlockSpec(memory_space=pltpu.HBM), whole],
        out_shape=[
            pltpu.HBM(tokens.shape, tokens.dtype),
            jax.ShapeDtypeStruct((heads, slots, head), jnp.bfloat16),
        ],
        scratch_shapes=[pltpu.SemaphoreType.DMA],
        cost_estimate=pl.CostEstimate(
            flops=2 * slots * width * width, bytes_accessed=2 * width * width, transcendentals=slots * width
        ),
        compiler_params=limit(8),
        name="project_query",
    )(tokens, w_query)


def own_kernel(scale, pieces, tokens_ref, query_ref, gain_ref, w_ref, gate_ref, own_ref, weights, sems):
    heads, _, head = query_ref.shape
    width = heads * head
    cols = width // pieces
    per = cols // head
    places = (0, 1, 3)

    def pull(piece, part):
        first = places[part] * width + piece * cols
        return pltpu.make_async_copy(
            w_ref.at[:, first : first + cols],
            weights.at[part, :, piece * cols : (piece + 1) * cols],
            sems.at[piece, part],
        )

    for piece in range(pieces):
        for part in (1, 2, 0):
            pull(piece, part).start()
    tokens = tokens_ref[...]

    def project(piece, part):
        pull(piece, part).wait()
        here = weights[part, :, piece * cols : (piece + 1) * cols]
        return silu(jnp.dot(tokens, here, preferred_element_type=jnp.float32))

    for piece in range(pieces):
        here = slice(piece * cols, (piece + 1) * cols)
        own_v = project(piece, 1).astype(jnp.bfloat16)
        own_k = project(piece, 2).astype(jnp.bfloat16)
        gate_ref[:, here] = (project(piece, 0) * gain_ref[:, here]).astype(gate_ref.dtype)
        for h in range(per):
            part = slice(h * head, (h + 1) * head)
            query = query_ref[piece * per + h].astype(jnp.float32)
            score = jnp.sum(query * own_k[:, part].astype(jnp.float32), axis=-1, keepdims=True) * scale
            weight = silu(score).astype(jnp.bfloat16).astype(jnp.float32)
            term = weight * own_v[:, part].astype(jnp.float32)
            own_ref[piece * per + h] = term.astype(own_ref.dtype)


def project_own(tokens, query, gain, w_uvqk, head):
    slots, width = tokens.shape
    heads = width // head
    pieces = 2
    whole = pl.BlockSpec(memory_space=pltpu.VMEM)
    return pl.pallas_call(
        functools.partial(own_kernel, head ** (-0.5), pieces),
        in_specs=[whole, whole, whole, pl.BlockSpec(memory_space=pltpu.HBM)],
        out_specs=[whole, whole],
        out_shape=[
            pltpu.VMEM((slots, width), jnp.bfloat16),
            pltpu.VMEM((heads, slots, head), jnp.bfloat16),
        ],
        scratch_shapes=[
            pltpu.VMEM((3, width, width), w_uvqk.dtype),
            pltpu.SemaphoreType.DMA((pieces, 3)),
        ],
        cost_estimate=pl.CostEstimate(
            flops=6 * slots * width * width, bytes_accessed=6 * width * width, transcendentals=3 * slots * width
        ),
        compiler_params=limit(14),
        name="project_own",
    )(tokens, query, gain.reshape(1, width), w_uvqk)


def visible_kernel(meta_ref, cache_ref, keys_ref, values_ref, sems):
    shards, length, head = keys_ref.shape
    visible = meta_ref[1]
    key_copy = pltpu.make_async_copy(cache_ref.at[:, 0], keys_ref, sems.at[0])
    value_copy = pltpu.make_async_copy(cache_ref.at[:, 1], values_ref, sems.at[1])
    key_copy.start()
    value_copy.start()
    key_copy.wait()
    for shard in range(shards):

        @pl.when(visible < (shard + 1) * length)
        def _():
            place = shard * length + lax.broadcasted_iota(jnp.int32, (length, head), 0)
            keys = keys_ref[shard].astype(jnp.float32)
            keys_ref[shard] = jnp.where(place < visible, keys, 0.0).astype(jnp.bfloat16)

    value_copy.wait()


def visible_prefix(meta, cache):
    shards, _, length, head = cache.shape
    kept = pltpu.VMEM((shards, length, head), cache.dtype)
    return pl.pallas_call(
        visible_kernel,
        in_specs=[pl.BlockSpec(memory_space=pltpu.SMEM), pl.BlockSpec(memory_space=pl.ANY)],
        out_specs=[pl.BlockSpec(memory_space=pltpu.VMEM), pl.BlockSpec(memory_space=pltpu.VMEM)],
        out_shape=[kept, kept],
        scratch_shapes=[pltpu.SemaphoreType.DMA((2,))],
        compiler_params=limit(1),
        name="visible_prefix",
    )(meta, cache)


def attend_kernel(scale, rows, query_ref, keys_ref, values_ref, out_ref):
    blocks, slots, head = query_ref.shape
    shards = keys_ref.shape[0]
    per = rows // slots

    def row_block(number, carry):
        first = number * per
        query = query_ref[pl.ds(first, per)].reshape(rows, head)
        query = (query.astype(jnp.float32) * (0.5 * scale)).astype(jnp.bfloat16)

        def scores(shard):
            return lax.dot_general(
                query, keys_ref[shard], (((1,), (1,)), ((), ())), preferred_element_type=jnp.float32
            )

        acc = jnp.zeros((rows, head), jnp.float32)
        ahead = scores(0)
        for shard in range(shards):
            half = ahead.astype(jnp.bfloat16)
            if shard + 1 < shards:
                ahead = scores(shard + 1)
            weight = half + half * jnp.tanh(half)
            acc = acc + jnp.dot(weight, values_ref[shard], preferred_element_type=jnp.float32)
        out_ref[pl.ds(first, per)] = acc.astype(jnp.bfloat16).reshape(per, slots, head)
        return carry

    lax.fori_loop(0, blocks // per, row_block, 0)


def attend(query, keys, values):
    blocks, slots, head = query.shape
    shards, length, _ = keys.shape
    rows = 4 * slots
    flops = 4 * blocks * slots * shards * length * head
    whole = pl.BlockSpec(memory_space=pltpu.VMEM)
    return pl.pallas_call(
        functools.partial(attend_kernel, head ** (-0.5), rows),
        in_specs=[whole, whole, whole],
        out_specs=whole,
        out_shape=jax.ShapeDtypeStruct(query.shape, jnp.bfloat16),
        cost_estimate=pl.CostEstimate(
            flops=flops, bytes_accessed=keys.size * 4, transcendentals=blocks * slots * shards * length
        ),
        compiler_params=limit(14),
        name="attend",
    )(query, keys, values)


def finish_kernel(pieces, facts_ref, mixed_ref, own_ref, gate_ref, w_ref, out_ref, buf, meta_ref, sems, sem):
    heads, slots, head = mixed_ref.shape
    facts = pltpu.make_async_copy(facts_ref, meta_ref, sem)
    facts.start()
    width = heads * head
    rows = slots // pieces
    copies = []
    for piece in range(pieces):
        here = slice(piece * rows, (piece + 1) * rows)
        mixed = jnp.concatenate(
            [
                mixed_ref[h, here].astype(jnp.float32) + own_ref[h, here].astype(jnp.float32)
                for h in range(heads)
            ],
            axis=1,
        )
        centre = mixed - jnp.sum(mixed, axis=-1, keepdims=True) * (1.0 / width)
        spread = jnp.sum(centre * centre, axis=-1, keepdims=True) * (1.0 / width)
        normed = centre * lax.rsqrt(spread + 1e-05) * gate_ref[here].astype(jnp.float32)
        result = jnp.dot(normed.astype(jnp.bfloat16), w_ref[...], preferred_element_type=jnp.float32)
        if piece == 0:
            facts.wait()
            count = meta_ref[0]
            first = meta_ref[2] * slots
        place = first + piece * rows + lax.broadcasted_iota(jnp.int32, result.shape, 0)
        buf[here] = jnp.where(place < count, result, 0.0).astype(jnp.bfloat16)
        copies.append(pltpu.make_async_copy(buf.at[here], out_ref.at[here], sems.at[piece]))
        copies[-1].start()
    for copy in copies:
        copy.wait()


def finish(meta, mixed, own, gate, w_output):
    slots, width = gate.shape
    pieces = 2
    whole = pl.BlockSpec(memory_space=pltpu.VMEM)
    return pl.pallas_call(
        functools.partial(finish_kernel, pieces),
        in_specs=[pl.BlockSpec(memory_space=pl.ANY)] + [whole] * 4,
        out_specs=pl.BlockSpec(memory_space=pltpu.HBM),
        scratch_shapes=[
            pltpu.VMEM((slots, width), jnp.bfloat16),
            pltpu.SMEM(meta.shape, meta.dtype),
            pltpu.SemaphoreType.DMA((pieces,)),
            pltpu.SemaphoreType.DMA,
        ],
        out_shape=jax.ShapeDtypeStruct((slots, width), jnp.bfloat16),
        cost_estimate=pl.CostEstimate(
            flops=2 * slots * width * width, bytes_accessed=2 * width * width, transcendentals=slots
        ),
        compiler_params=limit(10),
        name="finish",
    )(meta, mixed, own, gate, w_output)


def local(candidates, prefix_cache, w_uvqk, w_output, norm_gain, owner, counts, prefix_len):
    groups = lax.axis_size("group")
    group_here = lax.axis_index("group")
    helper_here = lax.axis_index("helper")
    offset = jnp.minimum(lax.optimization_barrier(owner[0]), groups - 1)
    width = candidates.shape[2]
    head = width // HEADS
    firsts, seconds, steps = plan(groups)
    first = pick_int([x for x, _ in steps], offset)
    second = pick_int([y for _, y in steps], offset)
    first_moves = [first_move(by, groups, head) for by in firsts]
    second_moves = [second_move(by, groups, head) for by in seconds]
    w_uvqk = pltpu.with_memory_space_constraint(w_uvqk, pltpu.HBM)
    prefix = pltpu.with_memory_space_constraint(prefix_cache[0], pltpu.HBM)
    tokens, split = lax.switch(first, first_moves, candidates[0], prefix)
    tokens, cache, query = lax.switch(second, second_moves, tokens, split, w_uvqk)
    user = (group_here - offset) % groups
    table = jnp.stack([counts, prefix_len, jnp.full_like(counts, helper_here)])
    places = lax.broadcasted_iota(jnp.int32, table.shape, 1)
    meta = jnp.sum(jnp.where(places == user, table, 0), axis=1)
    query_all = exchange(query)
    gate, own = project_own(tokens, query, norm_gain, w_uvqk, head)
    keys, values = visible_prefix(meta, cache)
    heads_out = attend(query_all, keys, values)
    mixed = exchange(heads_out)
    return finish(meta, mixed, own, gate, w_output)[None]


def solution(mesh):
    in_specs = (
        P("group", "helper", None),
        P("group", None, "helper", None),
        P(),
        P(),
        P(),
        P(),
        P(),
        P(),
    )
    out_specs = P("group", "helper", None)
    return jax.shard_map(local, mesh=mesh, in_specs=in_specs, out_specs=out_specs, check_vma=False)
```

```python
import functools

import jax
import jax.numpy as jnp
from jax import lax
from jax.experimental import pallas as pl
from jax.experimental.pallas import tpu as pltpu
from jax.sharding import PartitionSpec as P


HEADS = 8
FAR = 4


def silu(value):
    half = 0.5 * value
    return half + half * jnp.tanh(half)


def exchange(value):
    return lax.all_to_all(value, "helper", 0, 0, tiled=True)


def rotate(value, steps, count):
    if steps % count == 0:
        return value
    pairs = [(source, (source + steps) % count) for source in range(count)]
    return lax.ppermute(value, "group", pairs)


def first_move(steps, count, head):
    def move(tokens, cache):
        if steps == 0:
            split, moved = prepare(cache, head, tokens)
            return moved, split
        moved = rotate(tokens, steps, count)
        (split,) = prepare(cache, head)
        return moved, split

    return move


def second_move(steps, count, head):
    def move(tokens, split, w_uvqk):
        moved = rotate(tokens, steps, count)
        cache = exchange(split)
        w_query = fetch(w_uvqk)
        parts = 1 if abs(steps) > FAR else 2
        kept, query = project_query(moved, w_query, head, parts)
        return kept, cache, query

    return move


def plan(groups):
    steps = []
    for offset in range(groups):
        signed = (offset + groups // 2 - 1) % groups - groups // 2 + 1
        size, sign = abs(signed), 1 if signed > 0 else -1
        if size <= 2:
            steps.append((0, signed))
            continue
        far = groups // 2 if size >= groups // 2 - FAR else (size + (size < FAR)) // FAR * FAR
        steps.append((sign * (size - far), sign * far if far < groups // 2 else far))
    firsts = sorted({first for first, _ in steps})
    seconds = sorted({second for _, second in steps})
    return firsts, seconds, [(firsts.index(x), seconds.index(y)) for x, y in steps]


def pick_int(values, index):
    runs = []
    at = 0
    while at < len(values):
        slope = values[at + 1] - values[at] if at + 1 < len(values) else 0
        end = at + 1
        while end < len(values) and values[end] - values[end - 1] == slope:
            end += 1
        runs.append((at, values[at], slope))
        at = end
    out = None
    for start, value, slope in runs:
        line = value + slope * (index - start) if slope else jnp.int32(value)
        out = line if out is None else jnp.where(index >= start, line, out)
    return out


def limit(mebibytes):
    return pltpu.CompilerParams(vmem_limit_bytes=mebibytes << 20)


def prepare(cache, head, tokens=None):
    two, length, width = cache.shape
    heads = width // head
    shape = (heads, two, length, head)
    far = pl.BlockSpec(memory_space=pltpu.HBM)

    def kernel(*refs):
        if tokens is None:
            cache_ref, split_ref, buf, reads, writes = refs
        else:
            cache_ref, tokens_ref, split_ref, kept_ref, buf, reads, writes, held, moves = refs
            pull_tokens = pltpu.make_async_copy(tokens_ref, held, moves.at[0])
            push_tokens = pltpu.make_async_copy(held, kept_ref, moves.at[1])

        def pull(h):
            cols = pl.ds(pl.multiple_of(h * head, head), head)
            return pltpu.make_async_copy(cache_ref.at[:, :, cols], buf.at[h], reads.at[h])

        def push(h):
            return pltpu.make_async_copy(buf.at[h], split_ref.at[h], writes.at[h])

        def each(step):
            def body(h, carry):
                step(h)
                return carry

            lax.fori_loop(0, heads, body, 0)

        def pass_on(h):
            pull(h).wait()
            push(h).start()

        if tokens is not None:
            pull_tokens.start()
        each(lambda h: pull(h).start())
        if tokens is not None:
            pull_tokens.wait()
            push_tokens.start()
        each(pass_on)
        each(lambda h: push(h).wait())
        if tokens is not None:
            push_tokens.wait()

    operands = [cache]
    out_specs = [far]
    out_shape = [pltpu.HBM(shape, cache.dtype)]
    scratch = [
        pltpu.VMEM(shape, cache.dtype),
        pltpu.SemaphoreType.DMA((heads,)),
        pltpu.SemaphoreType.DMA((heads,)),
    ]
    if tokens is not None:
        operands.append(tokens)
        out_specs.append(far)
        out_shape.append(pltpu.HBM(tokens.shape, tokens.dtype))
        scratch += [pltpu.VMEM(tokens.shape, tokens.dtype), pltpu.SemaphoreType.DMA((2,))]
    return pl.pallas_call(
        kernel,
        in_specs=[far] * len(operands),
        out_specs=out_specs,
        out_shape=out_shape,
        scratch_shapes=scratch,
        compiler_params=limit(4),
        name="prepare",
    )(*operands)


def fetch_kernel(w_uvqk_ref, query_ref, sem):
    width = query_ref.shape[1]
    copy = pltpu.make_async_copy(w_uvqk_ref.at[:, 2 * width : 3 * width], query_ref, sem)
    copy.start()
    copy.wait()


def fetch(w_uvqk):
    width = w_uvqk.shape[0]
    return pl.pallas_call(
        fetch_kernel,
        in_specs=[pl.BlockSpec(memory_space=pltpu.HBM)],
        out_specs=pl.BlockSpec(memory_space=pltpu.VMEM),
        out_shape=pltpu.VMEM((width, width), w_uvqk.dtype),
        scratch_shapes=[pltpu.SemaphoreType.DMA],
        compiler_params=limit(1),
        name="fetch",
    )(w_uvqk)


def query_kernel(parts, tokens_ref, w_ref, kept_ref, out_ref, sem):
    heads, _, head = out_ref.shape
    keep = pltpu.make_async_copy(tokens_ref, kept_ref, sem)
    keep.start()
    tokens = tokens_ref[...]
    per = heads // parts

    def some_heads(part, carry):
        for h in range(0, per, 2):
            first = (part * per + h) * head
            cols = pl.ds(first if parts == 1 else pl.multiple_of(first, head), 2 * head)
            proj = jnp.dot(tokens, w_ref[:, cols], preferred_element_type=jnp.float32)
            proj = silu(proj).astype(jnp.bfloat16)
            out_ref[part * per + h] = proj[:, :head]
            out_ref[part * per + h + 1] = proj[:, head:]
        return carry

    if parts == 1:
        some_heads(0, 0)
    else:
        lax.fori_loop(0, parts, some_heads, 0)
    keep.wait()


def project_query(tokens, w_query, head, parts):
    slots, width = tokens.shape
    heads = width // head
    whole = pl.BlockSpec(memory_space=pltpu.VMEM)
    return pl.pallas_call(
        functools.partial(query_kernel, parts),
        in_specs=[whole, whole],
        out_specs=[pl.BlockSpec(memory_space=pltpu.HBM), whole],
        out_shape=[
            pltpu.HBM(tokens.shape, tokens.dtype),
            jax.ShapeDtypeStruct((heads, slots, head), jnp.bfloat16),
        ],
        scratch_shapes=[pltpu.SemaphoreType.DMA],
        cost_estimate=pl.CostEstimate(
            flops=2 * slots * width * width, bytes_accessed=2 * width * width, transcendentals=slots * width
        ),
        compiler_params=limit(8),
        name="project_query",
    )(tokens, w_query)


def own_kernel(scale, pieces, tokens_ref, query_ref, gain_ref, w_ref, gate_ref, own_ref, weights, sems):
    heads, _, head = query_ref.shape
    width = heads * head
    cols = width // pieces
    per = cols // head
    places = (0, 1, 3)

    def pull(piece, part):
        first = places[part] * width + piece * cols
        return pltpu.make_async_copy(
            w_ref.at[:, first : first + cols],
            weights.at[part, :, piece * cols : (piece + 1) * cols],
            sems.at[piece, part],
        )

    for piece in range(pieces):
        for part in (1, 2, 0):
            pull(piece, part).start()
    tokens = tokens_ref[...]

    def project(piece, part):
        pull(piece, part).wait()
        here = weights[part, :, piece * cols : (piece + 1) * cols]
        return silu(jnp.dot(tokens, here, preferred_element_type=jnp.float32))

    for piece in range(pieces):
        here = slice(piece * cols, (piece + 1) * cols)
        own_v = project(piece, 1).astype(jnp.bfloat16)
        own_k = project(piece, 2).astype(jnp.bfloat16)
        gate_ref[:, here] = (project(piece, 0) * gain_ref[:, here]).astype(gate_ref.dtype)
        for h in range(per):
            part = slice(h * head, (h + 1) * head)
            query = query_ref[piece * per + h].astype(jnp.float32)
            score = jnp.sum(query * own_k[:, part].astype(jnp.float32), axis=-1, keepdims=True) * scale
            weight = silu(score).astype(jnp.bfloat16).astype(jnp.float32)
            term = weight * own_v[:, part].astype(jnp.float32)
            own_ref[piece * per + h] = term.astype(own_ref.dtype)


def project_own(tokens, query, gain, w_uvqk, head):
    slots, width = tokens.shape
    heads = width // head
    pieces = 2
    whole = pl.BlockSpec(memory_space=pltpu.VMEM)
    return pl.pallas_call(
        functools.partial(own_kernel, head ** (-0.5), pieces),
        in_specs=[whole, whole, whole, pl.BlockSpec(memory_space=pltpu.HBM)],
        out_specs=[whole, whole],
        out_shape=[
            pltpu.VMEM((slots, width), jnp.bfloat16),
            pltpu.VMEM((heads, slots, head), jnp.bfloat16),
        ],
        scratch_shapes=[
            pltpu.VMEM((3, width, width), w_uvqk.dtype),
            pltpu.SemaphoreType.DMA((pieces, 3)),
        ],
        cost_estimate=pl.CostEstimate(
            flops=6 * slots * width * width, bytes_accessed=6 * width * width, transcendentals=3 * slots * width
        ),
        compiler_params=limit(14),
        name="project_own",
    )(tokens, query, gain.reshape(1, width), w_uvqk)


def visible_kernel(meta_ref, cache_ref, keys_ref, values_ref, sems):
    shards, length, head = keys_ref.shape
    visible = meta_ref[1]
    key_copy = pltpu.make_async_copy(cache_ref.at[:, 0], keys_ref, sems.at[0])
    value_copy = pltpu.make_async_copy(cache_ref.at[:, 1], values_ref, sems.at[1])
    key_copy.start()
    value_copy.start()
    key_copy.wait()
    for shard in range(shards):

        @pl.when(visible < (shard + 1) * length)
        def _():
            place = shard * length + lax.broadcasted_iota(jnp.int32, (length, head), 0)
            keys = keys_ref[shard].astype(jnp.float32)
            keys_ref[shard] = jnp.where(place < visible, keys, 0.0).astype(jnp.bfloat16)

    value_copy.wait()


def visible_prefix(meta, cache):
    shards, _, length, head = cache.shape
    kept = pltpu.VMEM((shards, length, head), cache.dtype)
    return pl.pallas_call(
        visible_kernel,
        in_specs=[pl.BlockSpec(memory_space=pltpu.SMEM), pl.BlockSpec(memory_space=pl.ANY)],
        out_specs=[pl.BlockSpec(memory_space=pltpu.VMEM), pl.BlockSpec(memory_space=pltpu.VMEM)],
        out_shape=[kept, kept],
        scratch_shapes=[pltpu.SemaphoreType.DMA((2,))],
        compiler_params=limit(1),
        name="visible_prefix",
    )(meta, cache)


def attend_kernel(scale, rows, query_ref, keys_ref, values_ref, out_ref):
    blocks, slots, head = query_ref.shape
    shards = keys_ref.shape[0]
    per = rows // slots

    for first in range(0, blocks, per):
        query = query_ref[first : first + per].reshape(rows, head)
        query = (query.astype(jnp.float32) * (0.5 * scale)).astype(jnp.bfloat16)

        def scores(shard):
            return lax.dot_general(
                query, keys_ref[shard], (((1,), (1,)), ((), ())), preferred_element_type=jnp.float32
            )

        acc = jnp.zeros((rows, head), jnp.float32)
        ahead = scores(0)
        for shard in range(shards):
            half = ahead.astype(jnp.bfloat16)
            if shard + 1 < shards:
                ahead = scores(shard + 1)
            weight = half + half * jnp.tanh(half)
            acc = acc + jnp.dot(weight, values_ref[shard], preferred_element_type=jnp.float32)
        out_ref[first : first + per] = acc.astype(jnp.bfloat16).reshape(per, slots, head)


def attend(query, keys, values):
    blocks, slots, head = query.shape
    shards, length, _ = keys.shape
    rows = 4 * slots
    flops = 4 * blocks * slots * shards * length * head
    whole = pl.BlockSpec(memory_space=pltpu.VMEM)
    return pl.pallas_call(
        functools.partial(attend_kernel, head ** (-0.5), rows),
        in_specs=[whole, whole, whole],
        out_specs=whole,
        out_shape=jax.ShapeDtypeStruct(query.shape, jnp.bfloat16),
        cost_estimate=pl.CostEstimate(
            flops=flops, bytes_accessed=keys.size * 4, transcendentals=blocks * slots * shards * length
        ),
        compiler_params=limit(14),
        name="attend",
    )(query, keys, values)


def finish_kernel(pieces, facts_ref, mixed_ref, own_ref, gate_ref, w_ref, out_ref, buf, meta_ref, sems, sem):
    heads, slots, head = mixed_ref.shape
    facts = pltpu.make_async_copy(facts_ref, meta_ref, sem)
    facts.start()
    width = heads * head
    rows = slots // pieces
    copies = []
    for piece in range(pieces):
        here = slice(piece * rows, (piece + 1) * rows)
        mixed = jnp.concatenate(
            [
                mixed_ref[h, here].astype(jnp.float32) + own_ref[h, here].astype(jnp.float32)
                for h in range(heads)
            ],
            axis=1,
        )
        centre = mixed - jnp.sum(mixed, axis=-1, keepdims=True) * (1.0 / width)
        spread = jnp.sum(centre * centre, axis=-1, keepdims=True) * (1.0 / width)
        normed = centre * lax.rsqrt(spread + 1e-05) * gate_ref[here].astype(jnp.float32)
        result = jnp.dot(normed.astype(jnp.bfloat16), w_ref[...], preferred_element_type=jnp.float32)
        if piece == 0:
            facts.wait()
            count = meta_ref[0]
            first = meta_ref[2] * slots
        place = first + piece * rows + lax.broadcasted_iota(jnp.int32, result.shape, 0)
        buf[here] = jnp.where(place < count, result, 0.0).astype(jnp.bfloat16)
        copies.append(pltpu.make_async_copy(buf.at[here], out_ref.at[here], sems.at[piece]))
        copies[-1].start()
    for copy in copies:
        copy.wait()


def finish(meta, mixed, own, gate, w_output):
    slots, width = gate.shape
    pieces = 2
    whole = pl.BlockSpec(memory_space=pltpu.VMEM)
    return pl.pallas_call(
        functools.partial(finish_kernel, pieces),
        in_specs=[pl.BlockSpec(memory_space=pl.ANY)] + [whole] * 4,
        out_specs=pl.BlockSpec(memory_space=pltpu.HBM),
        scratch_shapes=[
            pltpu.VMEM((slots, width), jnp.bfloat16),
            pltpu.SMEM(meta.shape, meta.dtype),
            pltpu.SemaphoreType.DMA((pieces,)),
            pltpu.SemaphoreType.DMA,
        ],
        out_shape=jax.ShapeDtypeStruct((slots, width), jnp.bfloat16),
        cost_estimate=pl.CostEstimate(
            flops=2 * slots * width * width, bytes_accessed=2 * width * width, transcendentals=slots
        ),
        compiler_params=limit(10),
        name="finish",
    )(meta, mixed, own, gate, w_output)


def local(candidates, prefix_cache, w_uvqk, w_output, norm_gain, owner, counts, prefix_len):
    groups = lax.axis_size("group")
    group_here = lax.axis_index("group")
    helper_here = lax.axis_index("helper")
    offset = jnp.minimum(lax.optimization_barrier(owner[0]), groups - 1)
    width = candidates.shape[2]
    head = width // HEADS
    firsts, seconds, steps = plan(groups)
    first = pick_int([x for x, _ in steps], offset)
    second = pick_int([y for _, y in steps], offset)
    first_moves = [first_move(by, groups, head) for by in firsts]
    second_moves = [second_move(by, groups, head) for by in seconds]
    w_uvqk = pltpu.with_memory_space_constraint(w_uvqk, pltpu.HBM)
    prefix = pltpu.with_memory_space_constraint(prefix_cache[0], pltpu.HBM)
    tokens, split = lax.switch(first, first_moves, candidates[0], prefix)
    tokens, cache, query = lax.switch(second, second_moves, tokens, split, w_uvqk)
    user = (group_here - offset) % groups
    table = jnp.stack([counts, prefix_len, jnp.full_like(counts, helper_here)])
    places = lax.broadcasted_iota(jnp.int32, table.shape, 1)
    meta = jnp.sum(jnp.where(places == user, table, 0), axis=1)
    query_all = exchange(query)
    gate, own = project_own(tokens, query, norm_gain, w_uvqk, head)
    keys, values = visible_prefix(meta, cache)
    heads_out = attend(query_all, keys, values)
    mixed = exchange(heads_out)
    return finish(meta, mixed, own, gate, w_output)[None]


def solution(mesh):
    in_specs = (
        P("group", "helper", None),
        P("group", None, "helper", None),
        P(),
        P(),
        P(),
        P(),
        P(),
        P(),
    )
    out_specs = P("group", "helper", None)
    return jax.shard_map(local, mesh=mesh, in_specs=in_specs, out_specs=out_specs, check_vma=False)
```

```python
import functools

import jax
import jax.numpy as jnp
from jax import lax
from jax.experimental import pallas as pl
from jax.experimental.pallas import tpu as pltpu
from jax.sharding import PartitionSpec as P


HEADS = 8
FAR = 4


def silu(value):
    half = 0.5 * value
    return half + half * jnp.tanh(half)


def exchange(value):
    return lax.all_to_all(value, "helper", 0, 0, tiled=True)


def rotate(value, steps, count):
    if steps % count == 0:
        return value
    pairs = [(source, (source + steps) % count) for source in range(count)]
    return lax.ppermute(value, "group", pairs)


def first_move(steps, count, head):
    def move(tokens, cache):
        if steps == 0:
            split, moved = prepare(cache, head, tokens)
            return moved, split
        moved = rotate(tokens, steps, count)
        (split,) = prepare(cache, head)
        return moved, split

    return move


def second_move(steps, count, head):
    def move(tokens, split, w_uvqk):
        moved = rotate(tokens, steps, count)
        cache = exchange(split)
        w_query = fetch(w_uvqk)
        parts = 1 if abs(steps) > FAR else 2
        kept, query = project_query(moved, w_query, head, parts)
        return kept, cache, query

    return move


def plan(groups):
    steps = []
    for offset in range(groups):
        signed = (offset + groups // 2 - 1) % groups - groups // 2 + 1
        size, sign = abs(signed), 1 if signed > 0 else -1
        if size <= 2:
            steps.append((0, signed))
            continue
        far = groups // 2 if size >= groups // 2 - FAR else (size + (size < 2 * FAR)) // FAR * FAR
        steps.append((sign * (size - far), sign * far if far < groups // 2 else far))
    firsts = sorted({first for first, _ in steps})
    seconds = sorted({second for _, second in steps})
    return firsts, seconds, [(firsts.index(x), seconds.index(y)) for x, y in steps]


def pick_int(values, index):
    runs = []
    at = 0
    while at < len(values):
        slope = values[at + 1] - values[at] if at + 1 < len(values) else 0
        end = at + 1
        while end < len(values) and values[end] - values[end - 1] == slope:
            end += 1
        runs.append((at, values[at], slope))
        at = end
    out = None
    for start, value, slope in runs:
        line = value + slope * (index - start) if slope else jnp.int32(value)
        out = line if out is None else jnp.where(index >= start, line, out)
    return out


def limit(mebibytes):
    return pltpu.CompilerParams(vmem_limit_bytes=mebibytes << 20)


def prepare(cache, head, tokens=None):
    two, length, width = cache.shape
    heads = width // head
    shape = (heads, two, length, head)
    far = pl.BlockSpec(memory_space=pltpu.HBM)

    def kernel(*refs):
        if tokens is None:
            cache_ref, split_ref, buf, reads, writes = refs
        else:
            cache_ref, tokens_ref, split_ref, kept_ref, buf, reads, writes, held, moves = refs
            pull_tokens = pltpu.make_async_copy(tokens_ref, held, moves.at[0])
            push_tokens = pltpu.make_async_copy(held, kept_ref, moves.at[1])

        def pull(h):
            cols = pl.ds(pl.multiple_of(h * head, head), head)
            return pltpu.make_async_copy(cache_ref.at[:, :, cols], buf.at[h], reads.at[h])

        def push(h):
            return pltpu.make_async_copy(buf.at[h], split_ref.at[h], writes.at[h])

        def each(step):
            def body(h, carry):
                step(h)
                return carry

            lax.fori_loop(0, heads, body, 0)

        def pass_on(h):
            pull(h).wait()
            push(h).start()

        if tokens is not None:
            pull_tokens.start()
        each(lambda h: pull(h).start())
        if tokens is not None:
            pull_tokens.wait()
            push_tokens.start()
        each(pass_on)
        each(lambda h: push(h).wait())
        if tokens is not None:
            push_tokens.wait()

    operands = [cache]
    out_specs = [far]
    out_shape = [pltpu.HBM(shape, cache.dtype)]
    scratch = [
        pltpu.VMEM(shape, cache.dtype),
        pltpu.SemaphoreType.DMA((heads,)),
        pltpu.SemaphoreType.DMA((heads,)),
    ]
    if tokens is not None:
        operands.append(tokens)
        out_specs.append(far)
        out_shape.append(pltpu.HBM(tokens.shape, tokens.dtype))
        scratch += [pltpu.VMEM(tokens.shape, tokens.dtype), pltpu.SemaphoreType.DMA((2,))]
    return pl.pallas_call(
        kernel,
        in_specs=[far] * len(operands),
        out_specs=out_specs,
        out_shape=out_shape,
        scratch_shapes=scratch,
        compiler_params=limit(4),
        name="prepare",
    )(*operands)


def fetch_kernel(w_uvqk_ref, query_ref, sem):
    width = query_ref.shape[1]
    copy = pltpu.make_async_copy(w_uvqk_ref.at[:, 2 * width : 3 * width], query_ref, sem)
    copy.start()
    copy.wait()


def fetch(w_uvqk):
    width = w_uvqk.shape[0]
    return pl.pallas_call(
        fetch_kernel,
        in_specs=[pl.BlockSpec(memory_space=pltpu.HBM)],
        out_specs=pl.BlockSpec(memory_space=pltpu.VMEM),
        out_shape=pltpu.VMEM((width, width), w_uvqk.dtype),
        scratch_shapes=[pltpu.SemaphoreType.DMA],
        compiler_params=limit(1),
        name="fetch",
    )(w_uvqk)


def query_kernel(parts, tokens_ref, w_ref, kept_ref, out_ref, sem):
    heads, _, head = out_ref.shape
    keep = pltpu.make_async_copy(tokens_ref, kept_ref, sem)
    keep.start()
    tokens = tokens_ref[...]
    per = heads // parts

    def some_heads(part, carry):
        for h in range(0, per, 2):
            first = (part * per + h) * head
            cols = pl.ds(first if parts == 1 else pl.multiple_of(first, head), 2 * head)
            proj = jnp.dot(tokens, w_ref[:, cols], preferred_element_type=jnp.float32)
            proj = silu(proj).astype(jnp.bfloat16)
            out_ref[part * per + h] = proj[:, :head]
            out_ref[part * per + h + 1] = proj[:, head:]
        return carry

    if parts == 1:
        some_heads(0, 0)
    else:
        lax.fori_loop(0, parts, some_heads, 0)
    keep.wait()


def project_query(tokens, w_query, head, parts):
    slots, width = tokens.shape
    heads = width // head
    whole = pl.BlockSpec(memory_space=pltpu.VMEM)
    return pl.pallas_call(
        functools.partial(query_kernel, parts),
        in_specs=[whole, whole],
        out_specs=[pl.BlockSpec(memory_space=pltpu.HBM), whole],
        out_shape=[
            pltpu.HBM(tokens.shape, tokens.dtype),
            jax.ShapeDtypeStruct((heads, slots, head), jnp.bfloat16),
        ],
        scratch_shapes=[pltpu.SemaphoreType.DMA],
        cost_estimate=pl.CostEstimate(
            flops=2 * slots * width * width, bytes_accessed=2 * width * width, transcendentals=slots * width
        ),
        compiler_params=limit(8),
        name="project_query",
    )(tokens, w_query)


def own_kernel(scale, pieces, tokens_ref, query_ref, gain_ref, w_ref, gate_ref, own_ref, weights, sems):
    heads, _, head = query_ref.shape
    width = heads * head
    cols = width // pieces
    per = cols // head
    places = (0, 1, 3)

    def pull(piece, part):
        first = places[part] * width + piece * cols
        return pltpu.make_async_copy(
            w_ref.at[:, first : first + cols],
            weights.at[part, :, piece * cols : (piece + 1) * cols],
            sems.at[piece, part],
        )

    for piece in range(pieces):
        for part in (1, 2, 0):
            pull(piece, part).start()
    tokens = tokens_ref[...]

    def project(piece, part):
        pull(piece, part).wait()
        here = weights[part, :, piece * cols : (piece + 1) * cols]
        return silu(jnp.dot(tokens, here, preferred_element_type=jnp.float32))

    for piece in range(pieces):
        here = slice(piece * cols, (piece + 1) * cols)
        own_v = project(piece, 1).astype(jnp.bfloat16)
        own_k = project(piece, 2).astype(jnp.bfloat16)
        gate_ref[:, here] = (project(piece, 0) * gain_ref[:, here]).astype(gate_ref.dtype)
        for h in range(per):
            part = slice(h * head, (h + 1) * head)
            query = query_ref[piece * per + h].astype(jnp.float32)
            score = jnp.sum(query * own_k[:, part].astype(jnp.float32), axis=-1, keepdims=True) * scale
            weight = silu(score).astype(jnp.bfloat16).astype(jnp.float32)
            term = weight * own_v[:, part].astype(jnp.float32)
            own_ref[piece * per + h] = term.astype(own_ref.dtype)


def project_own(tokens, query, gain, w_uvqk, head):
    slots, width = tokens.shape
    heads = width // head
    pieces = 2
    whole = pl.BlockSpec(memory_space=pltpu.VMEM)
    return pl.pallas_call(
        functools.partial(own_kernel, head ** (-0.5), pieces),
        in_specs=[whole, whole, whole, pl.BlockSpec(memory_space=pltpu.HBM)],
        out_specs=[whole, whole],
        out_shape=[
            pltpu.VMEM((slots, width), jnp.bfloat16),
            pltpu.VMEM((heads, slots, head), jnp.bfloat16),
        ],
        scratch_shapes=[
            pltpu.VMEM((3, width, width), w_uvqk.dtype),
            pltpu.SemaphoreType.DMA((pieces, 3)),
        ],
        cost_estimate=pl.CostEstimate(
            flops=6 * slots * width * width, bytes_accessed=6 * width * width, transcendentals=3 * slots * width
        ),
        compiler_params=limit(14),
        name="project_own",
    )(tokens, query, gain.reshape(1, width), w_uvqk)


def visible_kernel(meta_ref, cache_ref, keys_ref, values_ref, sems):
    shards, length, head = keys_ref.shape
    visible = meta_ref[1]
    key_copy = pltpu.make_async_copy(cache_ref.at[:, 0], keys_ref, sems.at[0])
    value_copy = pltpu.make_async_copy(cache_ref.at[:, 1], values_ref, sems.at[1])
    key_copy.start()
    value_copy.start()
    key_copy.wait()
    for shard in range(shards):

        @pl.when(visible < (shard + 1) * length)
        def _():
            place = shard * length + lax.broadcasted_iota(jnp.int32, (length, head), 0)
            keys = keys_ref[shard].astype(jnp.float32)
            keys_ref[shard] = jnp.where(place < visible, keys, 0.0).astype(jnp.bfloat16)

    value_copy.wait()


def visible_prefix(meta, cache):
    shards, _, length, head = cache.shape
    kept = pltpu.VMEM((shards, length, head), cache.dtype)
    return pl.pallas_call(
        visible_kernel,
        in_specs=[pl.BlockSpec(memory_space=pltpu.SMEM), pl.BlockSpec(memory_space=pl.ANY)],
        out_specs=[pl.BlockSpec(memory_space=pltpu.VMEM), pl.BlockSpec(memory_space=pltpu.VMEM)],
        out_shape=[kept, kept],
        scratch_shapes=[pltpu.SemaphoreType.DMA((2,))],
        compiler_params=limit(1),
        name="visible_prefix",
    )(meta, cache)


def attend_kernel(scale, rows, query_ref, keys_ref, values_ref, out_ref):
    blocks, slots, head = query_ref.shape
    shards = keys_ref.shape[0]
    per = rows // slots

    for first in range(0, blocks, per):
        query = query_ref[first : first + per].reshape(rows, head)
        query = (query.astype(jnp.float32) * (0.5 * scale)).astype(jnp.bfloat16)

        def scores(shard):
            return lax.dot_general(
                query, keys_ref[shard], (((1,), (1,)), ((), ())), preferred_element_type=jnp.float32
            )

        acc = jnp.zeros((rows, head), jnp.float32)
        ahead = scores(0)
        for shard in range(shards):
            half = ahead
            if shard + 1 < shards:
                ahead = scores(shard + 1)
            weight = (half + half * jnp.tanh(half)).astype(jnp.bfloat16)
            acc = acc + jnp.dot(weight, values_ref[shard], preferred_element_type=jnp.float32)
        out_ref[first : first + per] = acc.astype(jnp.bfloat16).reshape(per, slots, head)


def attend(query, keys, values):
    blocks, slots, head = query.shape
    shards, length, _ = keys.shape
    rows = 4 * slots
    flops = 4 * blocks * slots * shards * length * head
    whole = pl.BlockSpec(memory_space=pltpu.VMEM)
    return pl.pallas_call(
        functools.partial(attend_kernel, head ** (-0.5), rows),
        in_specs=[whole, whole, whole],
        out_specs=whole,
        out_shape=jax.ShapeDtypeStruct(query.shape, jnp.bfloat16),
        cost_estimate=pl.CostEstimate(
            flops=flops, bytes_accessed=keys.size * 4, transcendentals=blocks * slots * shards * length
        ),
        compiler_params=limit(14),
        name="attend",
    )(query, keys, values)


def finish_kernel(pieces, facts_ref, mixed_ref, own_ref, gate_ref, w_ref, out_ref, buf, meta_ref, sems, sem):
    heads, slots, head = mixed_ref.shape
    facts = pltpu.make_async_copy(facts_ref, meta_ref, sem)
    facts.start()
    width = heads * head
    rows = slots // pieces
    copies = []
    for piece in range(pieces):
        here = slice(piece * rows, (piece + 1) * rows)
        mixed = jnp.concatenate(
            [
                mixed_ref[h, here].astype(jnp.float32) + own_ref[h, here].astype(jnp.float32)
                for h in range(heads)
            ],
            axis=1,
        )
        centre = mixed - jnp.sum(mixed, axis=-1, keepdims=True) * (1.0 / width)
        spread = jnp.sum(centre * centre, axis=-1, keepdims=True) * (1.0 / width)
        normed = centre * lax.rsqrt(spread + 1e-05) * gate_ref[here].astype(jnp.float32)
        result = jnp.dot(normed.astype(jnp.bfloat16), w_ref[...], preferred_element_type=jnp.float32)
        if piece == 0:
            facts.wait()
            count = meta_ref[0]
            first = meta_ref[2] * slots
        place = first + piece * rows + lax.broadcasted_iota(jnp.int32, result.shape, 0)
        buf[here] = jnp.where(place < count, result, 0.0).astype(jnp.bfloat16)
        copies.append(pltpu.make_async_copy(buf.at[here], out_ref.at[here], sems.at[piece]))
        copies[-1].start()
    for copy in copies:
        copy.wait()


def finish(meta, mixed, own, gate, w_output):
    slots, width = gate.shape
    pieces = 2
    whole = pl.BlockSpec(memory_space=pltpu.VMEM)
    return pl.pallas_call(
        functools.partial(finish_kernel, pieces),
        in_specs=[pl.BlockSpec(memory_space=pl.ANY)] + [whole] * 4,
        out_specs=pl.BlockSpec(memory_space=pltpu.HBM),
        scratch_shapes=[
            pltpu.VMEM((slots, width), jnp.bfloat16),
            pltpu.SMEM(meta.shape, meta.dtype),
            pltpu.SemaphoreType.DMA((pieces,)),
            pltpu.SemaphoreType.DMA,
        ],
        out_shape=jax.ShapeDtypeStruct((slots, width), jnp.bfloat16),
        cost_estimate=pl.CostEstimate(
            flops=2 * slots * width * width, bytes_accessed=2 * width * width, transcendentals=slots
        ),
        compiler_params=limit(10),
        name="finish",
    )(meta, mixed, own, gate, w_output)


def local(candidates, prefix_cache, w_uvqk, w_output, norm_gain, owner, counts, prefix_len):
    groups = lax.axis_size("group")
    group_here = lax.axis_index("group")
    helper_here = lax.axis_index("helper")
    offset = jnp.minimum(lax.optimization_barrier(owner[0]), groups - 1)
    width = candidates.shape[2]
    head = width // HEADS
    firsts, seconds, steps = plan(groups)
    first = pick_int([x for x, _ in steps], offset)
    second = pick_int([y for _, y in steps], offset)
    first_moves = [first_move(by, groups, head) for by in firsts]
    second_moves = [second_move(by, groups, head) for by in seconds]
    w_uvqk = pltpu.with_memory_space_constraint(w_uvqk, pltpu.HBM)
    prefix = pltpu.with_memory_space_constraint(prefix_cache[0], pltpu.HBM)
    tokens, split = lax.switch(first, first_moves, candidates[0], prefix)
    tokens, cache, query = lax.switch(second, second_moves, tokens, split, w_uvqk)
    user = (group_here - offset) % groups
    table = jnp.stack([counts, prefix_len, jnp.full_like(counts, helper_here)])
    places = lax.broadcasted_iota(jnp.int32, table.shape, 1)
    meta = jnp.sum(jnp.where(places == user, table, 0), axis=1)
    query_all = exchange(query)
    gate, own = project_own(tokens, query, norm_gain, w_uvqk, head)
    keys, values = visible_prefix(meta, cache)
    heads_out = attend(query_all, keys, values)
    mixed = exchange(heads_out)
    return finish(meta, mixed, own, gate, w_output)[None]


def solution(mesh):
    in_specs = (
        P("group", "helper", None),
        P("group", None, "helper", None),
        P(),
        P(),
        P(),
        P(),
        P(),
        P(),
    )
    out_specs = P("group", "helper", None)
    return jax.shard_map(local, mesh=mesh, in_specs=in_specs, out_specs=out_specs, check_vma=False)
```
